32 devices in a mesh: gz: 8 (over z, y), pa: 4 (over x, core).
Axes of the slice: x: 2, y: 2, z: 4, core: 2. Of those that a mesh axis runs over, the one named last changes fastest.
Arguments:
- density: bfloat16 [64, 1024, 1024], P('gz', 'pa'), may hold values from -6 to 6
- green: float32 [128, 1024, 1024], P('gz', 'pa'), may hold values from 0.1 to 3
Outputs:
- potential: float32 [64, 1024, 1024], P('gz', 'pa')
The draws below stay inside these ranges and needn't reach their ends.
All inputs are finite; a program needn't handle non-finite values.
Results may differ from the reference program's by a relative error of at most 0.02.
Values may be sent and summed in bfloat16 or wider, within the bound.
A program may use at most 192 MiB of HBM per device.

```python
import math
import jax
import jax.numpy as jnp
from jax import lax

NX = 1024
NY = 1024
NZ = 64
M = 128
N_GZ = 8


def level_of(key, dims, cuts, least, high):
    level = 1.0
    for axis_at, shards_of in cuts:
        steps = jax.random.uniform(jax.random.fold_in(jax.random.fold_in(key, 6), axis_at), (shards_of,), jnp.float32, least / len(cuts), high / len(cuts))
        level = level * jnp.repeat(jnp.exp(steps), dims[axis_at] // shards_of).reshape((-1,) + (1,) * (len(dims) - 1 - axis_at))
    return level


def scatter_about(stream_key, extent, deviation, limit, cuts=(), kind=jnp.bfloat16):
    drawn = jax.random.normal(stream_key, extent, jnp.float32) * deviation
    if len(cuts) > 0:
        drawn = level_of(stream_key, extent, cuts, -0.22, 0.18) * drawn
    return jnp.clip(drawn, min=-limit, max=limit).astype(kind)


def setup_inputs(seed: int = 0) -> dict:
    arg_keys = jax.random.split(jax.random.key(seed), 3)
    return {
        "density": scatter_about(arg_keys[0], (NZ, NX, NY), 1.0, 6.0, ((0, 8), (1, 4))),
        "green": jnp.clip(jnp.exp(math.log(3.0) - 3.4011974 * jax.random.uniform(arg_keys[1], (M, NY, NX), jnp.float32) ** level_of(arg_keys[1], (M, NY, NX), ((0, 8), (1, 4)), -0.2, 0.2)), 0.1, 3.0),
    }


def cas_table(rows, cols, length):
    product = (rows[:, None] * cols[None, :]) % length
    angle = product.astype(jnp.float32) * (2.0 * math.pi / length)
    return (jnp.cos(angle) + jnp.sin(angle)).astype(jnp.bfloat16)


def blocked_sum(tables, pieces, rows, columns):
    def add_block(total, pair):
        table, piece = pair
        term = jnp.dot(table, piece, precision=lax.Precision.HIGHEST, preferred_element_type=jnp.float32).astype(jnp.bfloat16)
        term = lax.optimization_barrier(term)
        return total + term.astype(jnp.float32), None

    total, _ = lax.scan(add_block, jnp.zeros((rows, columns), jnp.float32), (tables, pieces))
    return total


def reference(density, green):
    z_cells, x_cells, y_cells = density.shape
    z_freqs = 2 * z_cells
    z_slab = z_cells // N_GZ
    k_block = z_freqs // N_GZ
    columns = x_cells * y_cells
    highest = lax.Precision.HIGHEST
    f_index = jnp.arange(z_freqs, dtype=jnp.int32)
    z_index = jnp.arange(z_cells, dtype=jnp.int32)
    forward_tables = cas_table(f_index, z_index, z_freqs).astype(jnp.float32).reshape(z_freqs, N_GZ, z_slab).transpose(1, 0, 2)
    slabs = density.astype(jnp.float32).reshape(N_GZ, z_slab, columns)
    zspec = blocked_sum(forward_tables, slabs, z_freqs, columns).astype(jnp.bfloat16).reshape(z_freqs, x_cells, y_cells)
    cas_y = cas_table(jnp.arange(y_cells, dtype=jnp.int32), jnp.arange(y_cells, dtype=jnp.int32), y_cells).astype(jnp.float32)
    cas_x = cas_table(jnp.arange(x_cells, dtype=jnp.int32), jnp.arange(x_cells, dtype=jnp.int32), x_cells).astype(jnp.float32)
    yspec = jnp.einsum('kxy,vy->kxv', zspec.astype(jnp.float32), cas_y, precision=highest).astype(jnp.bfloat16)
    xspec = jnp.einsum('kxv,ux->kvu', yspec.astype(jnp.float32), cas_x, precision=highest)
    weighted = (green * xspec).astype(jnp.bfloat16)
    yback = jnp.einsum('kvu,xu->kxv', weighted.astype(jnp.float32), cas_x, precision=highest).astype(jnp.bfloat16)
    zback = jnp.einsum('kxv,yv->kxy', yback.astype(jnp.float32), cas_y, precision=highest).astype(jnp.bfloat16)
    back_tables = cas_table(z_index, f_index, z_freqs).astype(jnp.float32).reshape(z_cells, N_GZ, k_block).transpose(1, 0, 2)
    blocks = zback.astype(jnp.float32).reshape(N_GZ, k_block, columns)
    total = blocked_sum(back_tables, blocks, z_cells, columns)
    scale = 1.0 / (x_cells * y_cells * z_freqs)
    return (total * scale).reshape(z_cells, x_cells, y_cells)
```

```python
import math

import jax
import jax.numpy as jnp
from jax import lax
from jax.experimental import pallas as pl
from jax.experimental.pallas import tpu as pltpu
from jax.sharding import PartitionSpec as P

BF = jnp.bfloat16
F32 = jnp.float32
CHUNKS = 2


def cas_table(rows, cols, length):
    product = rows[:, None] * cols[None, :] % length
    angle = product.astype(F32) * (2.0 * math.pi / length)
    return (jnp.cos(angle) + jnp.sin(angle)).astype(BF)


def square_table(n):
    index = jnp.arange(n, dtype=jnp.int32)
    return cas_table(index, index, n)


def cost(flops, *arrays):
    size = sum(math.prod(a.shape) * a.dtype.itemsize for a in arrays)
    return pl.CostEstimate(flops=flops, bytes_accessed=size, transcendentals=0)


def dot(a, b):
    return jnp.dot(a, b, preferred_element_type=F32)


def dot_t(a, b):
    return lax.dot_general(a, b, (((1,), (1,)), ((), ())), preferred_element_type=F32)


def on_rank(body, grid, in_specs, out_specs, out_shape, cost_estimate, **more):
    spec = pltpu.PrefetchScalarGridSpec(
        num_scalar_prefetch=1, grid=grid, in_specs=in_specs, out_specs=out_specs
    )
    return pl.pallas_call(
        lambda r, *refs: body(*refs),
        grid_spec=spec,
        out_shape=out_shape,
        cost_estimate=cost_estimate,
        **more,
    )


def green_piece(green, rank, step, groups):
    k, v, u = green.shape
    share = v // groups
    cut = math.gcd(k, 4)
    pieces = green.reshape(k, groups, share, u)

    def body(g_ref, o_ref):
        o_ref[...] = g_ref[:, 0].astype(BF)

    out = jax.ShapeDtypeStruct((k, share, u), BF)
    return on_rank(
        body,
        (k // cut,),
        [pl.BlockSpec((cut, 1, share, u), lambda i, r: (i, lax.rem(r[0] + step, groups), 0, 0))],
        pl.BlockSpec((cut, share, u), lambda i, r: (i, 0, 0)),
        out,
        cost(0, out, out, out),
    )(rank, pieces)


def shift(a, axis, step):
    n = lax.axis_size(axis)
    return lax.ppermute(a, axis, [(i, (i + step) % n) for i in range(n)])


def y_forward(density, table, pencils):
    z, x, y = density.shape
    block = y // pencils

    def body(d_ref, t_ref, o_ref):
        for p in range(pencils):
            rows = t_ref[p * block : (p + 1) * block, :]
            o_ref[p, 0] = dot_t(rows, d_ref[0]).astype(BF)

    out = jax.ShapeDtypeStruct((pencils, z, block, x), BF)
    return pl.pallas_call(
        body,
        grid=(z,),
        in_specs=[
            pl.BlockSpec((1, x, y), lambda i: (i, 0, 0)),
            pl.BlockSpec((y, y), lambda i: (0, 0)),
        ],
        out_specs=pl.BlockSpec((pencils, 1, block, x), lambda i: (0, i, 0, 0)),
        out_shape=out,
        cost_estimate=cost(2 * z * x * y * y, density, table, out),
        name="y_forward",
    )(density, table)


def x_forward(moved, table, groups):
    pencils, z, v, x = moved.shape
    u = pencils * x
    share = v // groups

    def body(m_ref, t_ref, o_ref):
        total = dot(m_ref[0, 0], t_ref[0:x, :])
        for p in range(1, pencils):
            total += dot(m_ref[p, 0], t_ref[p * x : (p + 1) * x, :])
        total = total.astype(BF)
        for j in range(groups):
            o_ref[j, 0] = total[j * share : (j + 1) * share, :]

    out = jax.ShapeDtypeStruct((groups, z, share, u), BF)
    return pl.pallas_call(
        body,
        grid=(z,),
        in_specs=[
            pl.BlockSpec((pencils, 1, v, x), lambda i: (0, i, 0, 0)),
            pl.BlockSpec((u, u), lambda i: (0, 0)),
        ],
        out_specs=pl.BlockSpec((groups, 1, share, u), lambda i: (0, i, 0, 0)),
        out_shape=out,
        cost_estimate=cost(2 * z * v * u * u, moved, table, out),
        name="x_forward",
    )(moved, table)


def z_weight(planes, greens, table, chunks):
    z, v, u = planes.shape
    groups = len(greens)
    part = greens[0].shape[0]
    k = part * groups
    depth = z // groups // chunks
    if v % 8:
        green = jnp.concatenate(greens, axis=0)
        spec = jnp.einsum("kz,zvu->kvu", table, planes, preferred_element_type=F32)
        weighted = (green.astype(F32) * spec).astype(BF)
        back = jnp.einsum("kz,kvu->zvu", table, weighted, preferred_element_type=F32).astype(BF)
        back = back.reshape(groups, chunks, depth, v, u)
        return [back[:, c] for c in range(chunks)]
    lanes = min(u, 512)
    rows = 16 if v % 16 == 0 else 8
    row = jnp.arange(8, dtype=jnp.int32)

    def widen(t):
        same = (jnp.arange(8 * t.shape[0]) % 8)[:, None] == (jnp.arange(8 * t.shape[1]) % 8)[None]
        return jnp.where(same, jnp.repeat(jnp.repeat(t, 8, axis=0), 8, axis=1), 0).astype(BF)

    wide = widen(table)
    tall = widen(table.T)

    def body(s_ref, *refs):
        g_refs, (w_ref, t_ref), o_refs = refs[:groups], refs[groups : groups + 2], refs[groups + 2 :]
        for i in range(0, rows, 8):
            flat = s_ref[:, i : i + 8, :].astype(F32).reshape(z * 8, lanes).astype(BF)
            spec = dot(w_ref[...], flat)
            weight = jnp.concatenate(
                [g[:, i : i + 8, :].astype(F32).reshape(part * 8, lanes) for g in g_refs], axis=0
            )
            back = dot(t_ref[...], (spec * weight).astype(BF))
            back = back.reshape(groups, chunks, depth, 8, lanes).astype(BF)
            for c in range(chunks):
                o_refs[c][:, :, i : i + 8, :] = back[:, c]

    out = jax.ShapeDtypeStruct((groups, depth, v, u), BF)
    at = lambda i, j: (0, i, j)
    whole = lambda i, j: (0, 0)
    return pl.pallas_call(
        body,
        grid=(v // rows, u // lanes),
        in_specs=[
            pl.BlockSpec((z, rows, lanes), at),
            *[pl.BlockSpec((part, rows, lanes), at)] * groups,
            pl.BlockSpec((k * 8, z * 8), whole),
            pl.BlockSpec((z * 8, k * 8), whole),
        ],
        out_specs=[pl.BlockSpec((groups, depth, rows, lanes), lambda i, j: (0, 0, i, j))] * chunks,
        out_shape=[out] * chunks,
        compiler_params=pltpu.CompilerParams(vmem_limit_bytes=60 * 2**20),
        cost_estimate=cost(32 * z * k * v * u, planes, *greens, planes),
        name="z_weight",
    )(planes, *greens, wide, tall)


def x_inverse(back, table, rank, step, pencils):
    groups, z, share, u = back.shape
    v = groups * share
    x = u // pencils

    def body(b_ref, t_ref, o_ref):
        rows = jnp.concatenate([b_ref[j, 0] for j in range(groups)], axis=0)
        o_ref[0] = dot_t(t_ref[...], rows).astype(BF)

    out = jax.ShapeDtypeStruct((z, x, v), BF)
    return on_rank(
        body,
        (z,),
        [
            pl.BlockSpec((groups, 1, share, u), lambda i, r: (0, i, 0, 0)),
            pl.BlockSpec((x, u), lambda i, r: (lax.rem(r[0] + step, pencils), 0)),
        ],
        pl.BlockSpec((1, x, v), lambda i, r: (i, 0, 0)),
        out,
        cost(2 * z * v * u * x, back, out),
    )(rank, back, table)


def y_inverse(returned, table, rank, scale, total, z_all, first):
    pencils = len(returned)
    z, x, v = returned[0].shape
    y = pencils * v

    def body(*refs):
        r_refs, t_refs, o_ref = refs[:pencils], refs[pencils : 2 * pencils], refs[-1]
        acc = dot(r_refs[0][0], t_refs[0][...])
        for p in range(1, pencils):
            acc += dot(r_refs[p][0], t_refs[p][...])
        o_ref[0] = acc * scale

    def rows_of(s):
        return lambda i, r: (lax.rem(r[0] + pencils - s, pencils), 0)

    specs = [pl.BlockSpec((1, x, v), lambda i, r: (i, 0, 0))] * pencils
    specs += [pl.BlockSpec((v, y), rows_of(s)) for s in range(pencils)]
    operands = [*returned, *[table] * pencils]
    aliases = {}
    if total is not None:
        aliases = {1 + len(operands): 0}
        specs.append(pl.BlockSpec(memory_space=pl.ANY))
        operands.append(total)
    return on_rank(
        body,
        (z,),
        specs,
        pl.BlockSpec((1, x, y), lambda i, r: (i + first, 0, 0)),
        jax.ShapeDtypeStruct((z_all, x, y), F32),
        cost(2 * z * x * y * y, *returned, *returned, *returned),
        input_output_aliases=aliases,
    )(rank, *operands)


def exchange(a, axis):
    return lax.all_to_all(a, axis, split_axis=0, concat_axis=0, tiled=True)


def staged(density, green):
    z_slab, _, y_cells = density.shape
    k_block, y_local, x_cells = green.shape
    groups = lax.axis_size("gz")
    pencils = lax.axis_size("pa")
    z_cells = z_slab * groups
    z_freqs = k_block * groups
    share = y_local // groups
    g_rank = lax.axis_index("gz").astype(jnp.int32)
    p_rank = lax.axis_index("pa").astype(jnp.int32)
    g_me, p_me = g_rank.reshape(1), p_rank.reshape(1)
    greens = []
    for s in [*range(1, groups), 0]:
        piece = green_piece(green, g_me, s, groups)
        if s:
            piece = shift(piece, "gz", s)
        greens.append(piece)
    order = jnp.array([*range(1, groups), 0], dtype=jnp.int32)
    sources = (g_rank - order) % groups
    f_index = (sources[:, None] * k_block + jnp.arange(k_block, dtype=jnp.int32)).reshape(-1)
    cas_y = square_table(y_cells)
    cas_x = cas_y if x_cells == y_cells else square_table(x_cells)
    cas_m = cas_table(f_index, jnp.arange(z_cells, dtype=jnp.int32), z_freqs)
    moved = y_forward(density, cas_y, pencils)
    moved = exchange(moved, "pa")
    planes = x_forward(moved, cas_x, groups)
    planes = exchange(planes, "gz").reshape(z_cells, share, x_cells)
    chunks = math.gcd(z_slab, CHUNKS)
    scale = 1.0 / (x_cells * y_cells * z_freqs)
    potential = None
    for c, back in enumerate(z_weight(planes, greens, cas_m, chunks)):
        back = exchange(back, "gz")
        returned = [x_inverse(back, cas_x, p_me, s, pencils) for s in range(pencils)]
        returned = [shift(a, "pa", s) if s else a for s, a in enumerate(returned)]
        first = c * (z_slab // chunks)
        potential = y_inverse(returned, cas_y, p_me, scale, potential, z_slab, first)
    return potential


MESH = pl.DeviceIdType.MESH
HALVES = 2


def fits(density, green, groups, pencils):
    zs, xl, y = density.shape
    kb, yl, u = green.shape
    power = all(v & (v - 1) == 0 for v in (y, kb * groups, groups))
    rows = yl // groups // HALVES
    return (
        power
        and groups > 1
        and pencils > 1
        and u == y
        and xl * pencils == u
        and yl * pencils == y
        and rows % 16 == 0
        and u % 512 == 0
        and xl % 128 == 0
        and (yl // HALVES) % 128 == 0
        and kb >= zs
    )


def cas_of(product, length):
    angle = (product & (length - 1)).astype(F32) * (2.0 * math.pi / length)
    return jnp.cos(angle) + jnp.sin(angle)


def spectral(density, green, groups, pencils):
    n, pens = groups, pencils
    zs, xl, y = density.shape
    kb, yl, u = green.shape
    z_all, k_all = zs * n, kb * n
    half = yl // HALVES
    rows = half // n
    lanes = 512
    strip = 32

    def kernel(d_hbm, g_hbm, ret, t_out, dens, stage, gsend, grecv, ysend, yrecv, psend, precv,
               brecv, xsend, table, wide, tall, load, gs, gr, ys, yr, ps, pr, bs, br, xs, xr, own):
        g = lax.axis_index("gz")
        p = lax.axis_index("pa")

        def gz_at(i):
            return lax.rem(g + 1 + lax.rem(i + n // 2 - 1, n - 1), n)

        def pa_at(i):
            return lax.rem(p + 1 + i, pens)

        def green_load(t):
            h, i = t // n, lax.rem(t, n)
            d = lax.rem(jnp.where(i < n - 1, gz_at(i), g), n)
            at = pl.multiple_of(h * half + d * rows, rows)
            return pltpu.make_async_copy(
                g_hbm.at[:, pl.ds(at, rows), :], stage.at[lax.rem(t, 2)], load.at[lax.rem(t, 2)]
            )

        def green_send(h, d):
            return pltpu.make_async_remote_copy(
                gsend.at[h, d], grecv.at[h, g], gs.at[h, d], gr.at[h, g],
                device_id={"gz": d}, device_id_type=MESH)

        def green_wait(h, s):
            pltpu.make_async_remote_copy(
                gsend.at[h, s], grecv.at[h, s], gs.at[h, s], gr.at[h, s],
                device_id={"gz": s}, device_id_type=MESH).wait_recv()

        def y_copy(z, q, to):
            return pltpu.make_async_remote_copy(
                ysend.at[q, z], yrecv.at[to, z], ys.at[q, z], yr.at[to, z],
                device_id={"pa": q}, device_id_type=MESH)

        def p_copy(h, d, to):
            return pltpu.make_async_remote_copy(
                psend.at[h, d], precv.at[h, to], ps.at[h, d], pr.at[h, to],
                device_id={"gz": d}, device_id_type=MESH)

        def b_copy(h, z, d, to):
            return pltpu.make_async_remote_copy(
                gsend.at[h, d, z], brecv.at[h, z, to], bs.at[h, z, d], br.at[h, z, to],
                device_id={"gz": d}, device_id_type=MESH)

        def x_copy(h, z, q, to):
            at = pl.multiple_of(to * yl + h * half, half)
            return pltpu.make_async_remote_copy(
                xsend.at[h, z, q], ret.at[z, :, pl.ds(at, half)], xs.at[h, z, q], xr.at[h, z, to],
                device_id={"pa": q}, device_id_type=MESH)

        def x_own(h, z):
            at = pl.multiple_of(p * yl + h * half, half)
            return pltpu.make_async_copy(
                xsend.at[h, z, p], ret.at[z, :, pl.ds(at, half)], own.at[h, z])

        fill = pltpu.make_async_copy(d_hbm, dens, load.at[2])
        green_load(0).start()
        green_load(1).start()
        fill.start()
        barrier = pltpu.get_barrier_semaphore()

        @pl.loop(0, n - 1)
        def _(i):
            pl.semaphore_signal(barrier, inc=1, device_id={"gz": gz_at(i)}, device_id_type=MESH)

        @pl.loop(0, pens - 1)
        def _(i):
            pl.semaphore_signal(barrier, inc=1, device_id={"pa": pa_at(i)}, device_id_type=MESH)

        pl.semaphore_wait(barrier, n + pens - 2)

        @pl.loop(0, HALVES * n)
        def _(t):
            h, i = t // n, lax.rem(t, n)
            slot = lax.rem(t, 2)
            green_load(t).wait()

            @pl.when(i < n - 1)
            def _():
                d = gz_at(i)
                gsend[h, d] = stage[slot].astype(BF)
                green_send(h, d).start()

            @pl.when(i == n - 1)
            def _():
                grecv[h, g] = stage[slot].astype(BF)

            @pl.when(t < HALVES * n - 2)
            def _():
                green_load(t + 2).start()

        @pl.loop(0, y // strip)
        def _(b):
            row = lax.broadcasted_iota(jnp.int32, (strip, y), 0) + b * strip
            col = lax.broadcasted_iota(jnp.int32, (strip, y), 1)
            table[pl.ds(pl.multiple_of(b * strip, strip), strip), :] = cas_of(row * col, y).astype(BF)

        keep = pltpu.make_async_copy(table, t_out, load.at[3])
        keep.start()
        fill.wait()

        @pl.loop(0, zs)
        def _(z):
            for q in range(pens):
                ysend[q, z] = dot_t(table[q * yl : (q + 1) * yl, :], dens[z]).astype(BF)

            @pl.loop(0, pens - 1)
            def _(i):
                y_copy(z, pa_at(i), p).start()

            yrecv[p, z] = ysend[p, z]

        def widen(ref):
            shape = (strip, ref.shape[1])

            @pl.loop(0, ref.shape[0] // strip)
            def _(b):
                row = lax.broadcasted_iota(jnp.int32, shape, 0) + b * strip
                col = lax.broadcasted_iota(jnp.int32, shape, 1)
                value = cas_of((row >> 3) * (col >> 3), k_all)
                same = (row & 7) == (col & 7)
                ref[pl.ds(pl.multiple_of(b * strip, strip), strip), :] = jnp.where(same, value, 0.0).astype(BF)

        widen(wide)
        widen(tall)

        @pl.loop(0, zs)
        def _(z):
            @pl.loop(0, pens - 1)
            def _(i):
                s = pa_at(i)
                y_copy(z, s, s).wait_recv()

            total = dot(yrecv[0, z], table[0:xl, :])
            for q in range(1, pens):
                total += dot(yrecv[q, z], table[q * xl : (q + 1) * xl, :])
            total = total.astype(BF)
            for h in range(HALVES):
                for d in range(n):
                    at = h * half + d * rows
                    psend[h, d, z] = total[at : at + rows, :]

        for h in range(HALVES):
            @pl.loop(0, n - 1)
            def _(i):
                p_copy(h, gz_at(i), g).start()

            precv[h, g] = psend[h, g]

        for h in range(HALVES):
            @pl.loop(0, n - 1)
            def _(i):
                d = gz_at(i)
                green_send(h, d).wait_send()

        for h in range(HALVES):
            @pl.loop(0, n - 1)
            def _(i):
                s = gz_at(i)
                green_wait(h, s)
                p_copy(h, s, s).wait_recv()

            @pl.loop(0, u // lanes)
            def _(c):
                at = pl.ds(pl.multiple_of(c * lanes, lanes), lanes)
                for r in range(0, rows, 8):
                    part = slice(r, r + 8)
                    flat = precv[h, :, :, part, at].astype(F32).reshape(z_all * 8, lanes).astype(BF)
                    spec = dot(wide[...], flat)
                    weight = grecv[h, :, :, part, at].astype(F32).reshape(k_all * 8, lanes)
                    back = dot(tall[...], (spec * weight).astype(BF))
                    gsend[h, :, :zs, part, at] = back.reshape(n, zs, 8, lanes).astype(BF)

            @pl.loop(0, zs)
            def _(z):
                @pl.loop(0, n - 1)
                def _(i):
                    b_copy(h, z, gz_at(i), g).start()

                brecv[h, z, g] = gsend[h, g, z]

        @pl.loop(0, HALVES * zs)
        def _(t):
            h, z = t // zs, lax.rem(t, zs)

            @pl.loop(0, n - 1)
            def _(i):
                s = gz_at(i)
                b_copy(h, z, s, s).wait_recv()

            rows_in = brecv[h, z].reshape(half, u)
            for q in range(pens):
                xsend[h, z, q] = dot_t(table[q * xl : (q + 1) * xl, :], rows_in).astype(BF)

            @pl.loop(0, pens - 1)
            def _(i):
                x_copy(h, z, pa_at(i), p).start()

            x_own(h, z).start()

        keep.wait()

        @pl.loop(0, zs)
        def _(z):
            @pl.loop(0, pens - 1)
            def _(i):
                y_copy(z, pa_at(i), p).wait_send()

        @pl.loop(0, HALVES)
        def _(h):
            @pl.loop(0, n - 1)
            def _(i):
                p_copy(h, gz_at(i), g).wait_send()

        @pl.loop(0, HALVES * zs)
        def _(t):
            h, z = t // zs, lax.rem(t, zs)

            @pl.loop(0, n - 1)
            def _(i):
                b_copy(h, z, gz_at(i), g).wait_send()

            @pl.loop(0, pens - 1)
            def _(i):
                s = pa_at(i)
                x_copy(h, z, s, p).wait_send()
                x_copy(h, z, s, s).wait_recv()

            x_own(h, z).wait()

    sems = pltpu.SemaphoreType.DMA
    return pl.pallas_call(
        kernel,
        out_shape=[
            jax.ShapeDtypeStruct((zs, xl, y), BF),
            jax.ShapeDtypeStruct((y, y), BF),
        ],
        in_specs=[pl.BlockSpec(memory_space=pl.ANY)] * 2,
        out_specs=[pl.BlockSpec(memory_space=pl.ANY)] * 2,
        scratch_shapes=[
            pltpu.VMEM((zs, xl, y), BF),
            pltpu.VMEM((2, kb, rows, u), F32),
            pltpu.VMEM((HALVES, n, kb, rows, u), BF),
            pltpu.VMEM((HALVES, n, kb, rows, u), BF),
            pltpu.VMEM((pens, zs, yl, xl), BF),
            pltpu.VMEM((pens, zs, yl, xl), BF),
            pltpu.VMEM((HALVES, n, zs, rows, u), BF),
            pltpu.VMEM((HALVES, n, zs, rows, u), BF),
            pltpu.VMEM((HALVES, zs, n, rows, u), BF),
            pltpu.VMEM((HALVES, zs, pens, xl, half), BF),
            pltpu.VMEM((y, y), BF),
            pltpu.VMEM((k_all * 8, z_all * 8), BF),
            pltpu.VMEM((z_all * 8, k_all * 8), BF),
            sems((4,)),
            sems((HALVES, n)),
            sems((HALVES, n)),
            sems((pens, zs)),
            sems((pens, zs)),
            sems((HALVES, n)),
            sems((HALVES, n)),
            sems((HALVES, zs, n)),
            sems((HALVES, zs, n)),
            sems((HALVES, zs, pens)),
            sems((HALVES, zs, pens)),
            sems((HALVES, zs)),
        ],
        compiler_params=pltpu.CompilerParams(
            collective_id=0, has_side_effects=True, vmem_limit_bytes=67_000_000
        ),
        name="spectral",
    )(density, green)


def y_finish(returned, table, scale):
    z, x, y = returned.shape

    def body(r_ref, t_ref, o_ref):
        o_ref[0] = dot(r_ref[0], t_ref[...]) * scale

    return pl.pallas_call(
        body,
        grid=(z,),
        in_specs=[
            pl.BlockSpec((1, x, y), lambda i: (i, 0, 0)),
            pl.BlockSpec((y, y), lambda i: (0, 0)),
        ],
        out_specs=pl.BlockSpec((1, x, y), lambda i: (i, 0, 0)),
        out_shape=jax.ShapeDtypeStruct((z, x, y), F32),
        cost_estimate=cost(2 * z * x * y * y, returned, returned, returned),
        name="y_finish",
    )(returned, table)


def local(density, green):
    groups = lax.axis_size("gz")
    pencils = lax.axis_size("pa")
    if not fits(density, green, groups, pencils):
        return staged(density, green)
    scale = 1.0 / (green.shape[2] * density.shape[2] * green.shape[0] * groups)
    returned, table = spectral(density, green, groups, pencils)
    return y_finish(returned, table, scale)


def solution(mesh):
    return jax.shard_map(
        local,
        mesh=mesh,
        in_specs=(P("gz", "pa", None), P("gz", "pa", None)),
        out_specs=P("gz", "pa", None),
        check_vma=False,
    )
```

```python
import math

import jax
import jax.numpy as jnp
from jax import lax
from jax.experimental import pallas as pl
from jax.experimental.pallas import tpu as pltpu
from jax.sharding import PartitionSpec as P

BF = jnp.bfloat16
F32 = jnp.float32
CHUNKS = 2


def cas_table(rows, cols, length):
    product = rows[:, None] * cols[None, :] % length
    angle = product.astype(F32) * (2.0 * math.pi / length)
    return (jnp.cos(angle) + jnp.sin(angle)).astype(BF)


def square_table(n):
    index = jnp.arange(n, dtype=jnp.int32)
    return cas_table(index, index, n)


def cost(flops, *arrays):
    size = sum(math.prod(a.shape) * a.dtype.itemsize for a in arrays)
    return pl.CostEstimate(flops=flops, bytes_accessed=size, transcendentals=0)


def dot(a, b):
    return jnp.dot(a, b, preferred_element_type=F32)


def dot_t(a, b):
    return lax.dot_general(a, b, (((1,), (1,)), ((), ())), preferred_element_type=F32)


def on_rank(body, grid, in_specs, out_specs, out_shape, cost_estimate, **more):
    spec = pltpu.PrefetchScalarGridSpec(
        num_scalar_prefetch=1, grid=grid, in_specs=in_specs, out_specs=out_specs
    )
    return pl.pallas_call(
        lambda r, *refs: body(*refs),
        grid_spec=spec,
        out_shape=out_shape,
        cost_estimate=cost_estimate,
        **more,
    )


def green_piece(green, rank, step, groups):
    k, v, u = green.shape
    share = v // groups
    cut = math.gcd(k, 4)
    pieces = green.reshape(k, groups, share, u)

    def body(g_ref, o_ref):
        o_ref[...] = g_ref[:, 0].astype(BF)

    out = jax.ShapeDtypeStruct((k, share, u), BF)
    return on_rank(
        body,
        (k // cut,),
        [pl.BlockSpec((cut, 1, share, u), lambda i, r: (i, lax.rem(r[0] + step, groups), 0, 0))],
        pl.BlockSpec((cut, share, u), lambda i, r: (i, 0, 0)),
        out,
        cost(0, out, out, out),
    )(rank, pieces)


def shift(a, axis, step):
    n = lax.axis_size(axis)
    return lax.ppermute(a, axis, [(i, (i + step) % n) for i in range(n)])


def y_forward(density, table, pencils):
    z, x, y = density.shape
    block = y // pencils

    def body(d_ref, t_ref, o_ref):
        for p in range(pencils):
            rows = t_ref[p * block : (p + 1) * block, :]
            o_ref[p, 0] = dot_t(rows, d_ref[0]).astype(BF)

    out = jax.ShapeDtypeStruct((pencils, z, block, x), BF)
    return pl.pallas_call(
        body,
        grid=(z,),
        in_specs=[
            pl.BlockSpec((1, x, y), lambda i: (i, 0, 0)),
            pl.BlockSpec((y, y), lambda i: (0, 0)),
        ],
        out_specs=pl.BlockSpec((pencils, 1, block, x), lambda i: (0, i, 0, 0)),
        out_shape=out,
        cost_estimate=cost(2 * z * x * y * y, density, table, out),
        name="y_forward",
    )(density, table)


def x_forward(moved, table, groups):
    pencils, z, v, x = moved.shape
    u = pencils * x
    share = v // groups

    def body(m_ref, t_ref, o_ref):
        total = dot(m_ref[0, 0], t_ref[0:x, :])
        for p in range(1, pencils):
            total += dot(m_ref[p, 0], t_ref[p * x : (p + 1) * x, :])
        total = total.astype(BF)
        for j in range(groups):
            o_ref[j, 0] = total[j * share : (j + 1) * share, :]

    out = jax.ShapeDtypeStruct((groups, z, share, u), BF)
    return pl.pallas_call(
        body,
        grid=(z,),
        in_specs=[
            pl.BlockSpec((pencils, 1, v, x), lambda i: (0, i, 0, 0)),
            pl.BlockSpec((u, u), lambda i: (0, 0)),
        ],
        out_specs=pl.BlockSpec((groups, 1, share, u), lambda i: (0, i, 0, 0)),
        out_shape=out,
        cost_estimate=cost(2 * z * v * u * u, moved, table, out),
        name="x_forward",
    )(moved, table)


def z_weight(planes, greens, table, chunks):
    z, v, u = planes.shape
    groups = len(greens)
    part = greens[0].shape[0]
    k = part * groups
    depth = z // groups // chunks
    if v % 8:
        green = jnp.concatenate(greens, axis=0)
        spec = jnp.einsum("kz,zvu->kvu", table, planes, preferred_element_type=F32)
        weighted = (green.astype(F32) * spec).astype(BF)
        back = jnp.einsum("kz,kvu->zvu", table, weighted, preferred_element_type=F32).astype(BF)
        back = back.reshape(groups, chunks, depth, v, u)
        return [back[:, c] for c in range(chunks)]
    lanes = min(u, 512)
    rows = 16 if v % 16 == 0 else 8
    row = jnp.arange(8, dtype=jnp.int32)

    def widen(t):
        same = (jnp.arange(8 * t.shape[0]) % 8)[:, None] == (jnp.arange(8 * t.shape[1]) % 8)[None]
        return jnp.where(same, jnp.repeat(jnp.repeat(t, 8, axis=0), 8, axis=1), 0).astype(BF)

    wide = widen(table)
    tall = widen(table.T)

    def body(s_ref, *refs):
        g_refs, (w_ref, t_ref), o_refs = refs[:groups], refs[groups : groups + 2], refs[groups + 2 :]
        for i in range(0, rows, 8):
            flat = s_ref[:, i : i + 8, :].astype(F32).reshape(z * 8, lanes).astype(BF)
            spec = dot(w_ref[...], flat)
            weight = jnp.concatenate(
                [g[:, i : i + 8, :].astype(F32).reshape(part * 8, lanes) for g in g_refs], axis=0
            )
            back = dot(t_ref[...], (spec * weight).astype(BF))
            back = back.reshape(groups, chunks, depth, 8, lanes).astype(BF)
            for c in range(chunks):
                o_refs[c][:, :, i : i + 8, :] = back[:, c]

    out = jax.ShapeDtypeStruct((groups, depth, v, u), BF)
    at = lambda i, j: (0, i, j)
    whole = lambda i, j: (0, 0)
    return pl.pallas_call(
        body,
        grid=(v // rows, u // lanes),
        in_specs=[
            pl.BlockSpec((z, rows, lanes), at),
            *[pl.BlockSpec((part, rows, lanes), at)] * groups,
            pl.BlockSpec((k * 8, z * 8), whole),
            pl.BlockSpec((z * 8, k * 8), whole),
        ],
        out_specs=[pl.BlockSpec((groups, depth, rows, lanes), lambda i, j: (0, 0, i, j))] * chunks,
        out_shape=[out] * chunks,
        compiler_params=pltpu.CompilerParams(vmem_limit_bytes=60 * 2**20),
        cost_estimate=cost(32 * z * k * v * u, planes, *greens, planes),
        name="z_weight",
    )(planes, *greens, wide, tall)


def x_inverse(back, table, rank, step, pencils):
    groups, z, share, u = back.shape
    v = groups * share
    x = u // pencils

    def body(b_ref, t_ref, o_ref):
        rows = jnp.concatenate([b_ref[j, 0] for j in range(groups)], axis=0)
        o_ref[0] = dot_t(t_ref[...], rows).astype(BF)

    out = jax.ShapeDtypeStruct((z, x, v), BF)
    return on_rank(
        body,
        (z,),
        [
            pl.BlockSpec((groups, 1, share, u), lambda i, r: (0, i, 0, 0)),
            pl.BlockSpec((x, u), lambda i, r: (lax.rem(r[0] + step, pencils), 0)),
        ],
        pl.BlockSpec((1, x, v), lambda i, r: (i, 0, 0)),
        out,
        cost(2 * z * v * u * x, back, out),
    )(rank, back, table)


def y_inverse(returned, table, rank, scale, total, z_all, first):
    pencils = len(returned)
    z, x, v = returned[0].shape
    y = pencils * v

    def body(*refs):
        r_refs, t_refs, o_ref = refs[:pencils], refs[pencils : 2 * pencils], refs[-1]
        acc = dot(r_refs[0][0], t_refs[0][...])
        for p in range(1, pencils):
            acc += dot(r_refs[p][0], t_refs[p][...])
        o_ref[0] = acc * scale

    def rows_of(s):
        return lambda i, r: (lax.rem(r[0] + pencils - s, pencils), 0)

    specs = [pl.BlockSpec((1, x, v), lambda i, r: (i, 0, 0))] * pencils
    specs += [pl.BlockSpec((v, y), rows_of(s)) for s in range(pencils)]
    operands = [*returned, *[table] * pencils]
    aliases = {}
    if total is not None:
        aliases = {1 + len(operands): 0}
        specs.append(pl.BlockSpec(memory_space=pl.ANY))
        operands.append(total)
    return on_rank(
        body,
        (z,),
        specs,
        pl.BlockSpec((1, x, y), lambda i, r: (i + first, 0, 0)),
        jax.ShapeDtypeStruct((z_all, x, y), F32),
        cost(2 * z * x * y * y, *returned, *returned, *returned),
        input_output_aliases=aliases,
    )(rank, *operands)


def exchange(a, axis):
    return lax.all_to_all(a, axis, split_axis=0, concat_axis=0, tiled=True)


def staged(density, green):
    z_slab, _, y_cells = density.shape
    k_block, y_local, x_cells = green.shape
    groups = lax.axis_size("gz")
    pencils = lax.axis_size("pa")
    z_cells = z_slab * groups
    z_freqs = k_block * groups
    share = y_local // groups
    g_rank = lax.axis_index("gz").astype(jnp.int32)
    p_rank = lax.axis_index("pa").astype(jnp.int32)
    g_me, p_me = g_rank.reshape(1), p_rank.reshape(1)
    greens = []
    for s in [*range(1, groups), 0]:
        piece = green_piece(green, g_me, s, groups)
        if s:
            piece = shift(piece, "gz", s)
        greens.append(piece)
    order = jnp.array([*range(1, groups), 0], dtype=jnp.int32)
    sources = (g_rank - order) % groups
    f_index = (sources[:, None] * k_block + jnp.arange(k_block, dtype=jnp.int32)).reshape(-1)
    cas_y = square_table(y_cells)
    cas_x = cas_y if x_cells == y_cells else square_table(x_cells)
    cas_m = cas_table(f_index, jnp.arange(z_cells, dtype=jnp.int32), z_freqs)
    moved = y_forward(density, cas_y, pencils)
    moved = exchange(moved, "pa")
    planes = x_forward(moved, cas_x, groups)
    planes = exchange(planes, "gz").reshape(z_cells, share, x_cells)
    chunks = math.gcd(z_slab, CHUNKS)
    scale = 1.0 / (x_cells * y_cells * z_freqs)
    potential = None
    for c, back in enumerate(z_weight(planes, greens, cas_m, chunks)):
        back = exchange(back, "gz")
        returned = [x_inverse(back, cas_x, p_me, s, pencils) for s in range(pencils)]
        returned = [shift(a, "pa", s) if s else a for s, a in enumerate(returned)]
        first = c * (z_slab // chunks)
        potential = y_inverse(returned, cas_y, p_me, scale, potential, z_slab, first)
    return potential


MESH = pl.DeviceIdType.MESH
HALVES = 2
LATE = 2


def fits(density, green, groups, pencils):
    zs, xl, y = density.shape
    kb, yl, u = green.shape
    power = all(v & (v - 1) == 0 for v in (y, kb * groups, groups))
    rows = yl // groups // HALVES
    return (
        power
        and groups > 1
        and pencils > 1
        and u == y
        and xl * pencils == u
        and yl * pencils == y
        and rows % 16 == 0
        and u % 512 == 0
        and xl % 128 == 0
        and (yl // HALVES) % 128 == 0
        and kb >= zs
    )


def cas_of(product, length):
    angle = (product & (length - 1)).astype(F32) * (2.0 * math.pi / length)
    return jnp.cos(angle) + jnp.sin(angle)


def spectral(density, green, groups, pencils, scale):
    n, pens = groups, pencils
    zs, xl, y = density.shape
    kb, yl, u = green.shape
    z_all, k_all = zs * n, kb * n
    half = yl // HALVES
    rows = half // n
    lanes = 512
    strip = 32

    early = max(zs - LATE, 0)

    def kernel(d_hbm, g_hbm, out, t_out, dens, stage, gsend, grecv, ysend, yrecv, psend, precv,
               brecv, xsend, ret, ready, table, wide, tall, load, gs, gr, ys, yr, ps, pr, bs, br, xs, xr,
               own, done):
        g = lax.axis_index("gz")
        p = lax.axis_index("pa")

        def gz_at(i):
            return lax.rem(g + 1 + i, n)

        def pa_at(i):
            return lax.rem(p + 1 + i, pens)

        def green_load(t):
            h, i = t // n, lax.rem(t, n)
            at = pl.multiple_of(h * half + gz_at(i) * rows, rows)
            return pltpu.make_async_copy(
                g_hbm.at[:, pl.ds(at, rows), :], stage.at[lax.rem(t, 2)], load.at[lax.rem(t, 2)]
            )

        def green_cast(t):
            h, i = t // n, lax.rem(t, n)
            slot = lax.rem(t, 2)
            green_load(t).wait()

            @pl.when(i < n - 1)
            def _():
                gsend[h, gz_at(i)] = stage[slot].astype(BF)

            @pl.when(i == n - 1)
            def _():
                grecv[h, g] = stage[slot].astype(BF)

            @pl.when(t < HALVES * n - 2)
            def _():
                green_load(t + 2).start()

        def settle(ref, sem):
            pltpu.make_async_copy(ref, ref, sem).wait()

        def green_copy(h, d):
            return pltpu.make_async_remote_copy(
                gsend.at[h, d], grecv.at[h, g], gs, gr.at[h],
                device_id={"gz": d}, device_id_type=MESH)

        def y_copy(z, q):
            return pltpu.make_async_remote_copy(
                ysend.at[q, z], yrecv.at[p, z], ys, yr.at[z],
                device_id={"pa": q}, device_id_type=MESH)

        def p_copy(h, d):
            return pltpu.make_async_remote_copy(
                psend.at[h, d], precv.at[h, g], ps, pr.at[h],
                device_id={"gz": d}, device_id_type=MESH)

        def b_copy(h, z, d):
            return pltpu.make_async_remote_copy(
                gsend.at[h, d, z], brecv.at[h, z, g], bs, br.at[h, z],
                device_id={"gz": d}, device_id_type=MESH)

        def x_at(h):
            return pl.ds(pl.multiple_of(p * yl + h * half, half), half)

        def x_copy(h, z, q, to):
            return pltpu.make_async_remote_copy(
                xsend.at[h, z, q], to.at[z, :, x_at(h)], xs, xr.at[z],
                device_id={"pa": q}, device_id_type=MESH)

        def x_own(h, z):
            return pltpu.make_async_copy(xsend.at[h, z, p], out.at[z, :, x_at(h)], own.at[h, z - early])

        def y_back(z):
            settle(ret.at[z, :, 0 : (pens - 1) * yl], xr.at[z])
            slot = lax.rem(z, 2)

            @pl.when(z >= 2)
            def _():
                settle(ready.at[slot], done.at[slot])

            ready[slot] = (dot(ret[z], table[...]) * scale).astype(BF)
            pltpu.make_async_copy(ready.at[slot], out.at[z], done.at[slot]).start()

        fill = pltpu.make_async_copy(d_hbm, dens, load.at[2])
        green_load(0).start()
        green_load(1).start()
        fill.start()
        barrier = pltpu.get_barrier_semaphore()

        @pl.loop(0, n - 1)
        def _(i):
            pl.semaphore_signal(barrier, inc=1, device_id={"gz": gz_at(i)}, device_id_type=MESH)

        @pl.loop(0, pens - 1)
        def _(i):
            pl.semaphore_signal(barrier, inc=1, device_id={"pa": pa_at(i)}, device_id_type=MESH)

        green_cast(jnp.int32(0))
        pl.semaphore_wait(barrier, n + pens - 2)

        @pl.loop(0, HALVES * n)
        def _(t):
            h, i = t // n, lax.rem(t, n)

            @pl.when(i < n - 1)
            def _():
                green_copy(h, gz_at(i)).start()

            @pl.when(t < HALVES * n - 1)
            def _():
                green_cast(t + 1)

        @pl.loop(0, y // strip)
        def _(b):
            row = lax.broadcasted_iota(jnp.int32, (strip, y), 0) + b * strip
            col = lax.broadcasted_iota(jnp.int32, (strip, y), 1)
            table[pl.ds(pl.multiple_of(b * strip, strip), strip), :] = cas_of(row * col, y).astype(BF)

        keep = pltpu.make_async_copy(table, t_out, load.at[3])
        keep.start()
        fill.wait()

        @pl.loop(0, zs)
        def _(z):
            for q in range(pens):
                ysend[q, z] = dot_t(table[q * yl : (q + 1) * yl, :], dens[z]).astype(BF)

            @pl.loop(0, pens - 1)
            def _(i):
                y_copy(z, pa_at(i)).start()

            yrecv[p, z] = ysend[p, z]

        def widen(ref):
            shape = (strip, ref.shape[1])

            @pl.loop(0, ref.shape[0] // strip)
            def _(b):
                row = lax.broadcasted_iota(jnp.int32, shape, 0) + b * strip
                col = lax.broadcasted_iota(jnp.int32, shape, 1)
                value = cas_of((row >> 3) * (col >> 3), k_all)
                same = (row & 7) == (col & 7)
                ref[pl.ds(pl.multiple_of(b * strip, strip), strip), :] = jnp.where(same, value, 0.0).astype(BF)

        widen(wide)
        widen(tall)

        @pl.loop(0, zs)
        def _(z):
            settle(yrecv.at[0 : pens - 1, z], yr.at[z])

            total = dot(yrecv[0, z], table[0:xl, :])
            for q in range(1, pens):
                total += dot(yrecv[q, z], table[q * xl : (q + 1) * xl, :])
            total = total.astype(BF)
            for h in range(HALVES):
                for d in range(n):
                    at = h * half + d * rows
                    psend[h, d, z] = total[at : at + rows, :]

        for h in range(HALVES):
            @pl.loop(0, n - 1)
            def _(i):
                p_copy(h, gz_at(i)).start()

            precv[h, g] = psend[h, g]

        settle(gsend.at[:, 0 : n - 1], gs)
        for h in range(HALVES):
            settle(grecv.at[h, 0 : n - 1], gr.at[h])
            settle(precv.at[h, 0 : n - 1], pr.at[h])

            @pl.loop(0, u // lanes)
            def _(c):
                at = pl.ds(pl.multiple_of(c * lanes, lanes), lanes)
                for r in range(0, rows, 8):
                    part = slice(r, r + 8)
                    flat = precv[h, :, :, part, at].astype(F32).reshape(z_all * 8, lanes).astype(BF)
                    spec = dot(wide[...], flat)
                    weight = grecv[h, :, :, part, at].astype(F32).reshape(k_all * 8, lanes)
                    back = dot(tall[...], (spec * weight).astype(BF))
                    gsend[h, :, :zs, part, at] = back.reshape(n, zs, 8, lanes).astype(BF)

            @pl.loop(0, zs)
            def _(z):
                @pl.loop(0, n - 1)
                def _(i):
                    b_copy(h, z, gz_at(i)).start()

                brecv[h, z, g] = gsend[h, g, z]

        @pl.loop(0, HALVES * zs)
        def _(t):
            h, z = t // zs, lax.rem(t, zs)
            settle(brecv.at[h, z, 0 : n - 1], br.at[h, z])
            rows_in = brecv[h, z].reshape(half, u)
            for q in range(pens):
                xsend[h, z, q] = dot_t(table[q * xl : (q + 1) * xl, :], rows_in).astype(BF)

            @pl.when(z < early)
            def _():
                @pl.loop(0, pens - 1)
                def _(i):
                    x_copy(h, z, pa_at(i), ret).start()

                ret[z, :, x_at(h)] = xsend[h, z, p]

            @pl.when(z >= early)
            def _():
                @pl.loop(0, pens - 1)
                def _(i):
                    x_copy(h, z, pa_at(i), out).start()

                x_own(h, z).start()

            @pl.when((h == HALVES - 1) & (z >= LATE))
            def _():
                y_back(z - LATE)

        keep.wait()
        settle(ysend.at[0 : pens - 1], ys)
        settle(psend.at[:, 0 : n - 1], ps)
        settle(gsend.at[:, 0 : n - 1, 0:zs], bs)
        settle(xsend.at[:, :, 0 : pens - 1], xs)
        for z in range(max(early - 2, 0), early):
            settle(ready.at[z % 2], done.at[z % 2])
        for z in range(early, zs):
            for h in range(HALVES):
                x_own(h, z).wait()
            settle(out.at[z, :, 0 : (pens - 1) * yl], xr.at[z])

    sems = pltpu.SemaphoreType.DMA
    return pl.pallas_call(
        kernel,
        out_shape=[
            jax.ShapeDtypeStruct((zs, xl, y), BF),
            jax.ShapeDtypeStruct((y, y), BF),
        ],
        in_specs=[pl.BlockSpec(memory_space=pl.ANY)] * 2,
        out_specs=[pl.BlockSpec(memory_space=pl.ANY)] * 2,
        scratch_shapes=[
            pltpu.VMEM((zs, xl, y), BF),
            pltpu.VMEM((2, kb, rows, u), F32),
            pltpu.VMEM((HALVES, n, kb, rows, u), BF),
            pltpu.VMEM((HALVES, n, kb, rows, u), BF),
            pltpu.VMEM((pens, zs, yl, xl), BF),
            pltpu.VMEM((pens, zs, yl, xl), BF),
            pltpu.VMEM((HALVES, n, zs, rows, u), BF),
            pltpu.VMEM((HALVES, n, zs, rows, u), BF),
            pltpu.VMEM((HALVES, zs, n, rows, u), BF),
            pltpu.VMEM((HALVES, zs, pens, xl, half), BF),
            pltpu.VMEM((max(early, 1), xl, y), BF),
            pltpu.VMEM((2, xl, y), BF),
            pltpu.VMEM((y, y), BF),
            pltpu.VMEM((k_all * 8, z_all * 8), BF),
            pltpu.VMEM((z_all * 8, k_all * 8), BF),
            sems((4,)),
            sems,
            sems((HALVES,)),
            sems,
            sems((zs,)),
            sems,
            sems((HALVES,)),
            sems,
            sems((HALVES, zs)),
            sems,
            sems((zs,)),
            sems((HALVES, zs - early)),
            sems((2,)),
        ],
        compiler_params=pltpu.CompilerParams(
            collective_id=0, has_side_effects=True, vmem_limit_bytes=67_000_000
        ),
        name="spectral",
    )(density, green)


def y_finish(mixed, table, scale):
    z, x, y = mixed.shape
    early = max(z - LATE, 0)
    order = [*range(early - early // 4), *range(early, z), *range(early - early // 4, early)]

    def body(m_hbm, t_hbm, o_hbm, held, table, made, fill, arrive, leave):
        def taken(i):
            return pltpu.make_async_copy(m_hbm.at[i], held.at[i], arrive.at[i])

        def given(i):
            return pltpu.make_async_copy(made.at[i], o_hbm.at[i], leave.at[i])

        lookup = pltpu.make_async_copy(t_hbm, table, fill)
        for at, i in enumerate(order):
            taken(i).start()
            if at == 0:
                lookup.start()
        for i in order:
            if i == early:
                lookup.wait()
            taken(i).wait()
            if i < early:
                made[i] = held[i].astype(F32)
            else:
                made[i] = dot(held[i], table[...]) * scale
            given(i).start()
        for i in order:
            given(i).wait()

    sems = pltpu.SemaphoreType.DMA
    return pl.pallas_call(
        body,
        in_specs=[pl.BlockSpec(memory_space=pl.ANY)] * 2,
        out_specs=pl.BlockSpec(memory_space=pl.ANY),
        out_shape=jax.ShapeDtypeStruct((z, x, y), F32),
        scratch_shapes=[
            pltpu.VMEM((z, x, y), BF),
            pltpu.VMEM((y, y), BF),
            pltpu.VMEM((z, x, y), F32),
            sems,
            sems((z,)),
            sems((z,)),
        ],
        cost_estimate=cost(2 * LATE * x * y * y, mixed, mixed, mixed),
        compiler_params=pltpu.CompilerParams(vmem_limit_bytes=67_000_000),
        name="y_finish",
    )(mixed, table)


def local(density, green):
    groups = lax.axis_size("gz")
    pencils = lax.axis_size("pa")
    if not fits(density, green, groups, pencils):
        return staged(density, green)
    scale = 1.0 / (green.shape[2] * density.shape[2] * green.shape[0] * groups)
    mixed, table = spectral(density, green, groups, pencils, scale)
    return y_finish(mixed, table, scale)


def solution(mesh):
    return jax.shard_map(
        local,
        mesh=mesh,
        in_specs=(P("gz", "pa", None), P("gz", "pa", None)),
        out_specs=P("gz", "pa", None),
        check_vma=False,
    )
```

```python
import math

import jax
import jax.numpy as jnp
from jax import lax
from jax.experimental import pallas as pl
from jax.experimental.pallas import tpu as pltpu
from jax.sharding import PartitionSpec as P

BF = jnp.bfloat16
F32 = jnp.float32
CHUNKS = 2


def cas_table(rows, cols, length):
    product = rows[:, None] * cols[None, :] % length
    angle = product.astype(F32) * (2.0 * math.pi / length)
    return (jnp.cos(angle) + jnp.sin(angle)).astype(BF)


def square_table(n):
    index = jnp.arange(n, dtype=jnp.int32)
    return cas_table(index, index, n)


def cost(flops, *arrays):
    size = sum(math.prod(a.shape) * a.dtype.itemsize for a in arrays)
    return pl.CostEstimate(flops=flops, bytes_accessed=size, transcendentals=0)


def dot(a, b):
    return jnp.dot(a, b, preferred_element_type=F32)


def dot_t(a, b):
    return lax.dot_general(a, b, (((1,), (1,)), ((), ())), preferred_element_type=F32)


def on_rank(body, grid, in_specs, out_specs, out_shape, cost_estimate, **more):
    spec = pltpu.PrefetchScalarGridSpec(
        num_scalar_prefetch=1, grid=grid, in_specs=in_specs, out_specs=out_specs
    )
    return pl.pallas_call(
        lambda r, *refs: body(*refs),
        grid_spec=spec,
        out_shape=out_shape,
        cost_estimate=cost_estimate,
        **more,
    )


def green_piece(green, rank, step, groups):
    k, v, u = green.shape
    share = v // groups
    cut = math.gcd(k, 4)
    pieces = green.reshape(k, groups, share, u)

    def body(g_ref, o_ref):
        o_ref[...] = g_ref[:, 0].astype(BF)

    out = jax.ShapeDtypeStruct((k, share, u), BF)
    return on_rank(
        body,
        (k // cut,),
        [pl.BlockSpec((cut, 1, share, u), lambda i, r: (i, lax.rem(r[0] + step, groups), 0, 0))],
        pl.BlockSpec((cut, share, u), lambda i, r: (i, 0, 0)),
        out,
        cost(0, out, out, out),
    )(rank, pieces)


def shift(a, axis, step):
    n = lax.axis_size(axis)
    return lax.ppermute(a, axis, [(i, (i + step) % n) for i in range(n)])


def y_forward(density, table, pencils):
    z, x, y = density.shape
    block = y // pencils

    def body(d_ref, t_ref, o_ref):
        for p in range(pencils):
            rows = t_ref[p * block : (p + 1) * block, :]
            o_ref[p, 0] = dot_t(rows, d_ref[0]).astype(BF)

    out = jax.ShapeDtypeStruct((pencils, z, block, x), BF)
    return pl.pallas_call(
        body,
        grid=(z,),
        in_specs=[
            pl.BlockSpec((1, x, y), lambda i: (i, 0, 0)),
            pl.BlockSpec((y, y), lambda i: (0, 0)),
        ],
        out_specs=pl.BlockSpec((pencils, 1, block, x), lambda i: (0, i, 0, 0)),
        out_shape=out,
        cost_estimate=cost(2 * z * x * y * y, density, table, out),
        name="y_forward",
    )(density, table)


def x_forward(moved, table, groups):
    pencils, z, v, x = moved.shape
    u = pencils * x
    share = v // groups

    def body(m_ref, t_ref, o_ref):
        total = dot(m_ref[0, 0], t_ref[0:x, :])
        for p in range(1, pencils):
            total += dot(m_ref[p, 0], t_ref[p * x : (p + 1) * x, :])
        total = total.astype(BF)
        for j in range(groups):
            o_ref[j, 0] = total[j * share : (j + 1) * share, :]

    out = jax.ShapeDtypeStruct((groups, z, share, u), BF)
    return pl.pallas_call(
        body,
        grid=(z,),
        in_specs=[
            pl.BlockSpec((pencils, 1, v, x), lambda i: (0, i, 0, 0)),
            pl.BlockSpec((u, u), lambda i: (0, 0)),
        ],
        out_specs=pl.BlockSpec((groups, 1, share, u), lambda i: (0, i, 0, 0)),
        out_shape=out,
        cost_estimate=cost(2 * z * v * u * u, moved, table, out),
        name="x_forward",
    )(moved, table)


def z_weight(planes, greens, table, chunks):
    z, v, u = planes.shape
    groups = len(greens)
    part = greens[0].shape[0]
    k = part * groups
    depth = z // groups // chunks
    if v % 8:
        green = jnp.concatenate(greens, axis=0)
        spec = jnp.einsum("kz,zvu->kvu", table, planes, preferred_element_type=F32)
        weighted = (green.astype(F32) * spec).astype(BF)
        back = jnp.einsum("kz,kvu->zvu", table, weighted, preferred_element_type=F32).astype(BF)
        back = back.reshape(groups, chunks, depth, v, u)
        return [back[:, c] for c in range(chunks)]
    lanes = min(u, 512)
    rows = 16 if v % 16 == 0 else 8
    row = jnp.arange(8, dtype=jnp.int32)

    def widen(t):
        same = (jnp.arange(8 * t.shape[0]) % 8)[:, None] == (jnp.arange(8 * t.shape[1]) % 8)[None]
        return jnp.where(same, jnp.repeat(jnp.repeat(t, 8, axis=0), 8, axis=1), 0).astype(BF)

    wide = widen(table)
    tall = widen(table.T)

    def body(s_ref, *refs):
        g_refs, (w_ref, t_ref), o_refs = refs[:groups], refs[groups : groups + 2], refs[groups + 2 :]
        for i in range(0, rows, 8):
            flat = s_ref[:, i : i + 8, :].astype(F32).reshape(z * 8, lanes).astype(BF)
            spec = dot(w_ref[...], flat)
            weight = jnp.concatenate(
                [g[:, i : i + 8, :].astype(F32).reshape(part * 8, lanes) for g in g_refs], axis=0
            )
            back = dot(t_ref[...], (spec * weight).astype(BF))
            back = back.reshape(groups, chunks, depth, 8, lanes).astype(BF)
            for c in range(chunks):
                o_refs[c][:, :, i : i + 8, :] = back[:, c]

    out = jax.ShapeDtypeStruct((groups, depth, v, u), BF)
    at = lambda i, j: (0, i, j)
    whole = lambda i, j: (0, 0)
    return pl.pallas_call(
        body,
        grid=(v // rows, u // lanes),
        in_specs=[
            pl.BlockSpec((z, rows, lanes), at),
            *[pl.BlockSpec((part, rows, lanes), at)] * groups,
            pl.BlockSpec((k * 8, z * 8), whole),
            pl.BlockSpec((z * 8, k * 8), whole),
        ],
        out_specs=[pl.BlockSpec((groups, depth, rows, lanes), lambda i, j: (0, 0, i, j))] * chunks,
        out_shape=[out] * chunks,
        compiler_params=pltpu.CompilerParams(vmem_limit_bytes=60 * 2**20),
        cost_estimate=cost(32 * z * k * v * u, planes, *greens, planes),
        name="z_weight",
    )(planes, *greens, wide, tall)


def x_inverse(back, table, rank, step, pencils):
    groups, z, share, u = back.shape
    v = groups * share
    x = u // pencils

    def body(b_ref, t_ref, o_ref):
        rows = jnp.concatenate([b_ref[j, 0] for j in range(groups)], axis=0)
        o_ref[0] = dot_t(t_ref[...], rows).astype(BF)

    out = jax.ShapeDtypeStruct((z, x, v), BF)
    return on_rank(
        body,
        (z,),
        [
            pl.BlockSpec((groups, 1, share, u), lambda i, r: (0, i, 0, 0)),
            pl.BlockSpec((x, u), lambda i, r: (lax.rem(r[0] + step, pencils), 0)),
        ],
        pl.BlockSpec((1, x, v), lambda i, r: (i, 0, 0)),
        out,
        cost(2 * z * v * u * x, back, out),
    )(rank, back, table)


def y_inverse(returned, table, rank, scale, total, z_all, first):
    pencils = len(returned)
    z, x, v = returned[0].shape
    y = pencils * v

    def body(*refs):
        r_refs, t_refs, o_ref = refs[:pencils], refs[pencils : 2 * pencils], refs[-1]
        acc = dot(r_refs[0][0], t_refs[0][...])
        for p in range(1, pencils):
            acc += dot(r_refs[p][0], t_refs[p][...])
        o_ref[0] = acc * scale

    def rows_of(s):
        return lambda i, r: (lax.rem(r[0] + pencils - s, pencils), 0)

    specs = [pl.BlockSpec((1, x, v), lambda i, r: (i, 0, 0))] * pencils
    specs += [pl.BlockSpec((v, y), rows_of(s)) for s in range(pencils)]
    operands = [*returned, *[table] * pencils]
    aliases = {}
    if total is not None:
        aliases = {1 + len(operands): 0}
        specs.append(pl.BlockSpec(memory_space=pl.ANY))
        operands.append(total)
    return on_rank(
        body,
        (z,),
        specs,
        pl.BlockSpec((1, x, y), lambda i, r: (i + first, 0, 0)),
        jax.ShapeDtypeStruct((z_all, x, y), F32),
        cost(2 * z * x * y * y, *returned, *returned, *returned),
        input_output_aliases=aliases,
    )(rank, *operands)


def exchange(a, axis):
    return lax.all_to_all(a, axis, split_axis=0, concat_axis=0, tiled=True)


def staged(density, green):
    z_slab, _, y_cells = density.shape
    k_block, y_local, x_cells = green.shape
    groups = lax.axis_size("gz")
    pencils = lax.axis_size("pa")
    z_cells = z_slab * groups
    z_freqs = k_block * groups
    share = y_local // groups
    g_rank = lax.axis_index("gz").astype(jnp.int32)
    p_rank = lax.axis_index("pa").astype(jnp.int32)
    g_me, p_me = g_rank.reshape(1), p_rank.reshape(1)
    greens = []
    for s in [*range(1, groups), 0]:
        piece = green_piece(green, g_me, s, groups)
        if s:
            piece = shift(piece, "gz", s)
        greens.append(piece)
    order = jnp.array([*range(1, groups), 0], dtype=jnp.int32)
    sources = (g_rank - order) % groups
    f_index = (sources[:, None] * k_block + jnp.arange(k_block, dtype=jnp.int32)).reshape(-1)
    cas_y = square_table(y_cells)
    cas_x = cas_y if x_cells == y_cells else square_table(x_cells)
    cas_m = cas_table(f_index, jnp.arange(z_cells, dtype=jnp.int32), z_freqs)
    moved = y_forward(density, cas_y, pencils)
    moved = exchange(moved, "pa")
    planes = x_forward(moved, cas_x, groups)
    planes = exchange(planes, "gz").reshape(z_cells, share, x_cells)
    chunks = math.gcd(z_slab, CHUNKS)
    scale = 1.0 / (x_cells * y_cells * z_freqs)
    potential = None
    for c, back in enumerate(z_weight(planes, greens, cas_m, chunks)):
        back = exchange(back, "gz")
        returned = [x_inverse(back, cas_x, p_me, s, pencils) for s in range(pencils)]
        returned = [shift(a, "pa", s) if s else a for s, a in enumerate(returned)]
        first = c * (z_slab // chunks)
        potential = y_inverse(returned, cas_y, p_me, scale, potential, z_slab, first)
    return potential


MESH = pl.DeviceIdType.MESH
HALVES = 2
LAG = 2


def fits(density, green, groups, pencils):
    zs, xl, y = density.shape
    kb, yl, u = green.shape
    power = all(v & (v - 1) == 0 for v in (y, kb * groups, groups))
    rows = yl // groups // HALVES
    return (
        power
        and groups > 1
        and pencils > 1
        and u == y
        and xl * pencils == u
        and yl * pencils == y
        and rows % 16 == 0
        and u % 512 == 0
        and xl % 128 == 0
        and (yl // HALVES) % 128 == 0
        and kb >= zs
    )


def cas_of(product, length):
    angle = (product & (length - 1)).astype(F32) * (2.0 * math.pi / length)
    return jnp.cos(angle) + jnp.sin(angle)


def spectral(density, green, groups, pencils, scale):
    n, pens = groups, pencils
    zs, xl, y = density.shape
    kb, yl, u = green.shape
    z_all, k_all = zs * n, kb * n
    half = yl // HALVES
    rows = half // n
    lanes = 512
    strip = 32

    lag = min(LAG, zs)
    others = [*range(1, pens - 1), 0] if pens > 2 else [0]

    def kernel(d_hbm, g_hbm, out, dens, stage, gsend, grecv, ysend, yrecv, psend, precv,
               brecv, xsend, ret, ready, table, wide, tall, load, gs, gr, ys, yr, ps, pr, bs, br, xs, xr,
               done):
        g = lax.axis_index("gz")
        p = lax.axis_index("pa")

        def gz_at(i):
            return lax.rem(g + 1 + i, n)

        def pa_at(i):
            return lax.rem(p + 1 + i, pens)

        def green_load(t):
            h, i = t // n, lax.rem(t, n)
            at = pl.multiple_of(h * half + gz_at(i) * rows, rows)
            return pltpu.make_async_copy(
                g_hbm.at[:, pl.ds(at, rows), :], stage.at[lax.rem(t, 2)], load.at[lax.rem(t, 2)]
            )

        def green_cast(t):
            h, i = t // n, lax.rem(t, n)
            slot = lax.rem(t, 2)
            green_load(t).wait()

            @pl.when(i < n - 1)
            def _():
                gsend[h, gz_at(i)] = stage[slot].astype(BF)

            @pl.when(i == n - 1)
            def _():
                grecv[h, g] = stage[slot].astype(BF)

            @pl.when(t < HALVES * n - 2)
            def _():
                green_load(t + 2).start()

        def settle(ref, sem):
            pltpu.make_async_copy(ref, ref, sem).wait()

        def green_copy(h, d):
            return pltpu.make_async_remote_copy(
                gsend.at[h, d], grecv.at[h, g], gs, gr.at[h],
                device_id={"gz": d}, device_id_type=MESH)

        def y_copy(z, q):
            return pltpu.make_async_remote_copy(
                ysend.at[q, z], yrecv.at[p, z], ys, yr.at[z],
                device_id={"pa": q}, device_id_type=MESH)

        def p_copy(h, d):
            return pltpu.make_async_remote_copy(
                psend.at[h, d], precv.at[h, g], ps, pr.at[h],
                device_id={"gz": d}, device_id_type=MESH)

        def b_copy(h, z, d):
            return pltpu.make_async_remote_copy(
                gsend.at[h, d, z], brecv.at[h, z, g], bs, br.at[h, z],
                device_id={"gz": d}, device_id_type=MESH)

        def x_at(h):
            return pl.ds(pl.multiple_of(p * yl + h * half, half), half)

        def x_copy(h, z, q):
            return pltpu.make_async_remote_copy(
                xsend.at[h, z, q], ret.at[z, :, x_at(h)], xs, xr.at[z],
                device_id={"pa": q}, device_id_type=MESH)

        def y_back(z):
            settle(ret.at[z, :, 0 : (pens - 1) * yl], xr.at[z])
            slot = lax.rem(z, 2)

            @pl.when(z >= 2)
            def _():
                settle(ready.at[slot], done.at[slot])

            ready[slot] = (dot(ret[z], table[...]) * scale).astype(BF)
            pltpu.make_async_copy(ready.at[slot], out.at[z], done.at[slot]).start()

        fill = pltpu.make_async_copy(d_hbm, dens, load.at[2])
        green_load(0).start()
        green_load(1).start()
        fill.start()
        barrier = pltpu.get_barrier_semaphore()

        @pl.loop(0, n - 1)
        def _(i):
            pl.semaphore_signal(barrier, inc=1, device_id={"gz": gz_at(i)}, device_id_type=MESH)

        @pl.loop(0, pens - 1)
        def _(i):
            pl.semaphore_signal(barrier, inc=1, device_id={"pa": pa_at(i)}, device_id_type=MESH)

        green_cast(jnp.int32(0))
        pl.semaphore_wait(barrier, n + pens - 2)

        @pl.loop(0, HALVES * n)
        def _(t):
            h, i = t // n, lax.rem(t, n)

            @pl.when(i < n - 1)
            def _():
                green_copy(h, gz_at(i)).start()

            @pl.when(t < HALVES * n - 1)
            def _():
                green_cast(t + 1)

        @pl.loop(0, y // strip)
        def _(b):
            row = lax.broadcasted_iota(jnp.int32, (strip, y), 0) + b * strip
            col = lax.broadcasted_iota(jnp.int32, (strip, y), 1)
            table[pl.ds(pl.multiple_of(b * strip, strip), strip), :] = cas_of(row * col, y).astype(BF)

        fill.wait()

        @pl.loop(0, zs)
        def _(z):
            for q in range(pens):
                ysend[q, z] = dot_t(table[q * yl : (q + 1) * yl, :], dens[z]).astype(BF)

            @pl.loop(0, pens - 1)
            def _(i):
                y_copy(z, pa_at(i)).start()

            yrecv[p, z] = ysend[p, z]

        def widen(ref):
            shape = (strip, ref.shape[1])

            @pl.loop(0, ref.shape[0] // strip)
            def _(b):
                row = lax.broadcasted_iota(jnp.int32, shape, 0) + b * strip
                col = lax.broadcasted_iota(jnp.int32, shape, 1)
                value = cas_of((row >> 3) * (col >> 3), k_all)
                same = (row & 7) == (col & 7)
                ref[pl.ds(pl.multiple_of(b * strip, strip), strip), :] = jnp.where(same, value, 0.0).astype(BF)

        widen(wide)
        widen(tall)

        @pl.loop(0, zs)
        def _(z):
            settle(yrecv.at[0 : pens - 1, z], yr.at[z])

            total = dot(yrecv[0, z], table[0:xl, :])
            for q in range(1, pens):
                total += dot(yrecv[q, z], table[q * xl : (q + 1) * xl, :])
            total = total.astype(BF)
            for h in range(HALVES):
                for d in range(n):
                    at = h * half + d * rows
                    psend[h, d, z] = total[at : at + rows, :]

        for h in range(HALVES):
            @pl.loop(0, n - 1)
            def _(i):
                p_copy(h, gz_at(i)).start()

            precv[h, g] = psend[h, g]

        settle(gsend.at[:, 0 : n - 1], gs)
        for h in range(HALVES):
            settle(grecv.at[h, 0 : n - 1], gr.at[h])
            settle(precv.at[h, 0 : n - 1], pr.at[h])

            @pl.loop(0, u // lanes)
            def _(c):
                at = pl.ds(pl.multiple_of(c * lanes, lanes), lanes)
                for r in range(0, rows, 8):
                    part = slice(r, r + 8)
                    flat = precv[h, :, :, part, at].astype(F32).reshape(z_all * 8, lanes).astype(BF)
                    spec = dot(wide[...], flat)
                    weight = grecv[h, :, :, part, at].astype(F32).reshape(k_all * 8, lanes)
                    back = dot(tall[...], (spec * weight).astype(BF))
                    gsend[h, :, :zs, part, at] = back.reshape(n, zs, 8, lanes).astype(BF)

            @pl.loop(0, zs)
            def _(z):
                @pl.loop(0, n - 1)
                def _(i):
                    b_copy(h, z, gz_at(i)).start()

                brecv[h, z, g] = gsend[h, g, z]

        @pl.loop(0, HALVES * zs)
        def _(t):
            h, z = t // zs, lax.rem(t, zs)
            settle(brecv.at[h, z, 0 : n - 1], br.at[h, z])
            rows_in = brecv[h, z].reshape(half, u)

            def piece(q):
                at = pl.ds(pl.multiple_of(q * xl, xl), xl)
                return dot_t(table[at, :], rows_in).astype(BF)

            for at, i in enumerate(others):
                xsend[h, z, pa_at(i)] = piece(pa_at(i))
                if at:
                    x_copy(h, z, pa_at(others[at - 1])).start()
            ret[z, :, x_at(h)] = piece(p)
            x_copy(h, z, pa_at(others[-1])).start()

            @pl.when((h == HALVES - 1) & (z >= lag))
            def _():
                y_back(z - lag)

        for z in range(zs - lag, zs):
            y_back(jnp.int32(z))
        settle(ysend.at[0 : pens - 1], ys)
        settle(psend.at[:, 0 : n - 1], ps)
        settle(gsend.at[:, 0 : n - 1, 0:zs], bs)
        settle(xsend.at[:, :, 0 : pens - 1], xs)
        for z in range(max(zs - 2, 0), zs):
            settle(ready.at[z % 2], done.at[z % 2])

    sems = pltpu.SemaphoreType.DMA
    return pl.pallas_call(
        kernel,
        out_shape=jax.ShapeDtypeStruct((zs, xl, y), BF),
        in_specs=[pl.BlockSpec(memory_space=pl.ANY)] * 2,
        out_specs=pl.BlockSpec(memory_space=pl.ANY),
        scratch_shapes=[
            pltpu.VMEM((zs, xl, y), BF),
            pltpu.VMEM((2, kb, rows, u), F32),
            pltpu.VMEM((HALVES, n, kb, rows, u), BF),
            pltpu.VMEM((HALVES, n, kb, rows, u), BF),
            pltpu.VMEM((pens, zs, yl, xl), BF),
            pltpu.VMEM((pens, zs, yl, xl), BF),
            pltpu.VMEM((HALVES, n, zs, rows, u), BF),
            pltpu.VMEM((HALVES, n, zs, rows, u), BF),
            pltpu.VMEM((HALVES, zs, n, rows, u), BF),
            pltpu.VMEM((HALVES, zs, pens, xl, half), BF),
            pltpu.VMEM((zs, xl, y), BF),
            pltpu.VMEM((2, xl, y), BF),
            pltpu.VMEM((y, y), BF),
            pltpu.VMEM((k_all * 8, z_all * 8), BF),
            pltpu.VMEM((z_all * 8, k_all * 8), BF),
            sems((3,)),
            sems,
            sems((HALVES,)),
            sems,
            sems((zs,)),
            sems,
            sems((HALVES,)),
            sems,
            sems((HALVES, zs)),
            sems,
            sems((zs,)),
            sems((2,)),
        ],
        compiler_params=pltpu.CompilerParams(
            collective_id=0, has_side_effects=True, vmem_limit_bytes=67_000_000
        ),
        name="spectral",
    )(density, green)


def widen_result(narrow):
    z, x, y = narrow.shape

    def body(n_hbm, o_hbm, held, made, arrive, leave):
        def taken(i):
            return pltpu.make_async_copy(n_hbm.at[i], held.at[i], arrive.at[i])

        def given(i):
            return pltpu.make_async_copy(made.at[i], o_hbm.at[i], leave.at[i])

        for i in range(z):
            taken(i).start()
        for i in range(z):
            taken(i).wait()
            made[i] = held[i].astype(F32)
            given(i).start()
        for i in range(z):
            given(i).wait()

    sems = pltpu.SemaphoreType.DMA
    return pl.pallas_call(
        body,
        in_specs=[pl.BlockSpec(memory_space=pl.ANY)],
        out_specs=pl.BlockSpec(memory_space=pl.ANY),
        out_shape=jax.ShapeDtypeStruct((z, x, y), F32),
        scratch_shapes=[
            pltpu.VMEM((z, x, y), BF),
            pltpu.VMEM((z, x, y), F32),
            sems((z,)),
            sems((z,)),
        ],
        compiler_params=pltpu.CompilerParams(vmem_limit_bytes=67_000_000),
        cost_estimate=cost(z * x * y, narrow, narrow, narrow),
        name="widen_result",
    )(narrow)


def local(density, green):
    groups = lax.axis_size("gz")
    pencils = lax.axis_size("pa")
    if not fits(density, green, groups, pencils):
        return staged(density, green)
    scale = 1.0 / (green.shape[2] * density.shape[2] * green.shape[0] * groups)
    return widen_result(spectral(density, green, groups, pencils, scale))


def solution(mesh):
    return jax.shard_map(
        local,
        mesh=mesh,
        in_specs=(P("gz", "pa", None), P("gz", "pa", None)),
        out_specs=P("gz", "pa", None),
        check_vma=False,
    )
```

```python
import math

import jax
import jax.numpy as jnp
from jax import lax
from jax.experimental import pallas as pl
from jax.experimental.pallas import tpu as pltpu
from jax.sharding import PartitionSpec as P

BF = jnp.bfloat16
F32 = jnp.float32
CHUNKS = 2


def cas_table(rows, cols, length):
    product = rows[:, None] * cols[None, :] % length
    angle = product.astype(F32) * (2.0 * math.pi / length)
    return (jnp.cos(angle) + jnp.sin(angle)).astype(BF)


def square_table(n):
    index = jnp.arange(n, dtype=jnp.int32)
    return cas_table(index, index, n)


def cost(flops, *arrays):
    size = sum(math.prod(a.shape) * a.dtype.itemsize for a in arrays)
    return pl.CostEstimate(flops=flops, bytes_accessed=size, transcendentals=0)


def dot(a, b):
    return jnp.dot(a, b, preferred_element_type=F32)


def dot_t(a, b):
    return lax.dot_general(a, b, (((1,), (1,)), ((), ())), preferred_element_type=F32)


def on_rank(body, grid, in_specs, out_specs, out_shape, cost_estimate, **more):
    spec = pltpu.PrefetchScalarGridSpec(
        num_scalar_prefetch=1, grid=grid, in_specs=in_specs, out_specs=out_specs
    )
    return pl.pallas_call(
        lambda r, *refs: body(*refs),
        grid_spec=spec,
        out_shape=out_shape,
        cost_estimate=cost_estimate,
        **more,
    )


def green_piece(green, rank, step, groups):
    k, v, u = green.shape
    share = v // groups
    cut = math.gcd(k, 4)
    pieces = green.reshape(k, groups, share, u)

    def body(g_ref, o_ref):
        o_ref[...] = g_ref[:, 0].astype(BF)

    out = jax.ShapeDtypeStruct((k, share, u), BF)
    return on_rank(
        body,
        (k // cut,),
        [pl.BlockSpec((cut, 1, share, u), lambda i, r: (i, lax.rem(r[0] + step, groups), 0, 0))],
        pl.BlockSpec((cut, share, u), lambda i, r: (i, 0, 0)),
        out,
        cost(0, out, out, out),
    )(rank, pieces)


def shift(a, axis, step):
    n = lax.axis_size(axis)
    return lax.ppermute(a, axis, [(i, (i + step) % n) for i in range(n)])


def y_forward(density, table, pencils):
    z, x, y = density.shape
    block = y // pencils

    def body(d_ref, t_ref, o_ref):
        for p in range(pencils):
            rows = t_ref[p * block : (p + 1) * block, :]
            o_ref[p, 0] = dot_t(rows, d_ref[0]).astype(BF)

    out = jax.ShapeDtypeStruct((pencils, z, block, x), BF)
    return pl.pallas_call(
        body,
        grid=(z,),
        in_specs=[
            pl.BlockSpec((1, x, y), lambda i: (i, 0, 0)),
            pl.BlockSpec((y, y), lambda i: (0, 0)),
        ],
        out_specs=pl.BlockSpec((pencils, 1, block, x), lambda i: (0, i, 0, 0)),
        out_shape=out,
        cost_estimate=cost(2 * z * x * y * y, density, table, out),
        name="y_forward",
    )(density, table)


def x_forward(moved, table, groups):
    pencils, z, v, x = moved.shape
    u = pencils * x
    share = v // groups

    def body(m_ref, t_ref, o_ref):
        total = dot(m_ref[0, 0], t_ref[0:x, :])
        for p in range(1, pencils):
            total += dot(m_ref[p, 0], t_ref[p * x : (p + 1) * x, :])
        total = total.astype(BF)
        for j in range(groups):
            o_ref[j, 0] = total[j * share : (j + 1) * share, :]

    out = jax.ShapeDtypeStruct((groups, z, share, u), BF)
    return pl.pallas_call(
        body,
        grid=(z,),
        in_specs=[
            pl.BlockSpec((pencils, 1, v, x), lambda i: (0, i, 0, 0)),
            pl.BlockSpec((u, u), lambda i: (0, 0)),
        ],
        out_specs=pl.BlockSpec((groups, 1, share, u), lambda i: (0, i, 0, 0)),
        out_shape=out,
        cost_estimate=cost(2 * z * v * u * u, moved, table, out),
        name="x_forward",
    )(moved, table)


def z_weight(planes, greens, table, chunks):
    z, v, u = planes.shape
    groups = len(greens)
    part = greens[0].shape[0]
    k = part * groups
    depth = z // groups // chunks
    if v % 8:
        green = jnp.concatenate(greens, axis=0)
        spec = jnp.einsum("kz,zvu->kvu", table, planes, preferred_element_type=F32)
        weighted = (green.astype(F32) * spec).astype(BF)
        back = jnp.einsum("kz,kvu->zvu", table, weighted, preferred_element_type=F32).astype(BF)
        back = back.reshape(groups, chunks, depth, v, u)
        return [back[:, c] for c in range(chunks)]
    lanes = min(u, 512)
    rows = 16 if v % 16 == 0 else 8
    row = jnp.arange(8, dtype=jnp.int32)

    def widen(t):
        same = (jnp.arange(8 * t.shape[0]) % 8)[:, None] == (jnp.arange(8 * t.shape[1]) % 8)[None]
        return jnp.where(same, jnp.repeat(jnp.repeat(t, 8, axis=0), 8, axis=1), 0).astype(BF)

    wide = widen(table)
    tall = widen(table.T)

    def body(s_ref, *refs):
        g_refs, (w_ref, t_ref), o_refs = refs[:groups], refs[groups : groups + 2], refs[groups + 2 :]
        for i in range(0, rows, 8):
            flat = s_ref[:, i : i + 8, :].astype(F32).reshape(z * 8, lanes).astype(BF)
            spec = dot(w_ref[...], flat)
            weight = jnp.concatenate(
                [g[:, i : i + 8, :].astype(F32).reshape(part * 8, lanes) for g in g_refs], axis=0
            )
            back = dot(t_ref[...], (spec * weight).astype(BF))
            back = back.reshape(groups, chunks, depth, 8, lanes).astype(BF)
            for c in range(chunks):
                o_refs[c][:, :, i : i + 8, :] = back[:, c]

    out = jax.ShapeDtypeStruct((groups, depth, v, u), BF)
    at = lambda i, j: (0, i, j)
    whole = lambda i, j: (0, 0)
    return pl.pallas_call(
        body,
        grid=(v // rows, u // lanes),
        in_specs=[
            pl.BlockSpec((z, rows, lanes), at),
            *[pl.BlockSpec((part, rows, lanes), at)] * groups,
            pl.BlockSpec((k * 8, z * 8), whole),
            pl.BlockSpec((z * 8, k * 8), whole),
        ],
        out_specs=[pl.BlockSpec((groups, depth, rows, lanes), lambda i, j: (0, 0, i, j))] * chunks,
        out_shape=[out] * chunks,
        compiler_params=pltpu.CompilerParams(vmem_limit_bytes=60 * 2**20),
        cost_estimate=cost(32 * z * k * v * u, planes, *greens, planes),
        name="z_weight",
    )(planes, *greens, wide, tall)


def x_inverse(back, table, rank, step, pencils):
    groups, z, share, u = back.shape
    v = groups * share
    x = u // pencils

    def body(b_ref, t_ref, o_ref):
        rows = jnp.concatenate([b_ref[j, 0] for j in range(groups)], axis=0)
        o_ref[0] = dot_t(t_ref[...], rows).astype(BF)

    out = jax.ShapeDtypeStruct((z, x, v), BF)
    return on_rank(
        body,
        (z,),
        [
            pl.BlockSpec((groups, 1, share, u), lambda i, r: (0, i, 0, 0)),
            pl.BlockSpec((x, u), lambda i, r: (lax.rem(r[0] + step, pencils), 0)),
        ],
        pl.BlockSpec((1, x, v), lambda i, r: (i, 0, 0)),
        out,
        cost(2 * z * v * u * x, back, out),
    )(rank, back, table)


def y_inverse(returned, table, rank, scale, total, z_all, first):
    pencils = len(returned)
    z, x, v = returned[0].shape
    y = pencils * v

    def body(*refs):
        r_refs, t_refs, o_ref = refs[:pencils], refs[pencils : 2 * pencils], refs[-1]
        acc = dot(r_refs[0][0], t_refs[0][...])
        for p in range(1, pencils):
            acc += dot(r_refs[p][0], t_refs[p][...])
        o_ref[0] = acc * scale

    def rows_of(s):
        return lambda i, r: (lax.rem(r[0] + pencils - s, pencils), 0)

    specs = [pl.BlockSpec((1, x, v), lambda i, r: (i, 0, 0))] * pencils
    specs += [pl.BlockSpec((v, y), rows_of(s)) for s in range(pencils)]
    operands = [*returned, *[table] * pencils]
    aliases = {}
    if total is not None:
        aliases = {1 + len(operands): 0}
        specs.append(pl.BlockSpec(memory_space=pl.ANY))
        operands.append(total)
    return on_rank(
        body,
        (z,),
        specs,
        pl.BlockSpec((1, x, y), lambda i, r: (i + first, 0, 0)),
        jax.ShapeDtypeStruct((z_all, x, y), F32),
        cost(2 * z * x * y * y, *returned, *returned, *returned),
        input_output_aliases=aliases,
    )(rank, *operands)


def exchange(a, axis):
    return lax.all_to_all(a, axis, split_axis=0, concat_axis=0, tiled=True)


def staged(density, green):
    z_slab, _, y_cells = density.shape
    k_block, y_local, x_cells = green.shape
    groups = lax.axis_size("gz")
    pencils = lax.axis_size("pa")
    z_cells = z_slab * groups
    z_freqs = k_block * groups
    share = y_local // groups
    g_rank = lax.axis_index("gz").astype(jnp.int32)
    p_rank = lax.axis_index("pa").astype(jnp.int32)
    g_me, p_me = g_rank.reshape(1), p_rank.reshape(1)
    greens = []
    for s in [*range(1, groups), 0]:
        piece = green_piece(green, g_me, s, groups)
        if s:
            piece = shift(piece, "gz", s)
        greens.append(piece)
    order = jnp.array([*range(1, groups), 0], dtype=jnp.int32)
    sources = (g_rank - order) % groups
    f_index = (sources[:, None] * k_block + jnp.arange(k_block, dtype=jnp.int32)).reshape(-1)
    cas_y = square_table(y_cells)
    cas_x = cas_y if x_cells == y_cells else square_table(x_cells)
    cas_m = cas_table(f_index, jnp.arange(z_cells, dtype=jnp.int32), z_freqs)
    moved = y_forward(density, cas_y, pencils)
    moved = exchange(moved, "pa")
    planes = x_forward(moved, cas_x, groups)
    planes = exchange(planes, "gz").reshape(z_cells, share, x_cells)
    chunks = math.gcd(z_slab, CHUNKS)
    scale = 1.0 / (x_cells * y_cells * z_freqs)
    potential = None
    for c, back in enumerate(z_weight(planes, greens, cas_m, chunks)):
        back = exchange(back, "gz")
        returned = [x_inverse(back, cas_x, p_me, s, pencils) for s in range(pencils)]
        returned = [shift(a, "pa", s) if s else a for s, a in enumerate(returned)]
        first = c * (z_slab // chunks)
        potential = y_inverse(returned, cas_y, p_me, scale, potential, z_slab, first)
    return potential


MESH = pl.DeviceIdType.MESH
HALVES = 2
LAG = 2


def fits(density, green, groups, pencils):
    zs, xl, y = density.shape
    kb, yl, u = green.shape
    power = all(v & (v - 1) == 0 for v in (y, kb * groups, groups))
    rows = yl // groups // HALVES
    return (
        power
        and groups > 1
        and pencils > 1
        and u == y
        and xl * pencils == u
        and yl * pencils == y
        and rows % 16 == 0
        and u % 512 == 0
        and xl % 128 == 0
        and (yl // HALVES) % 128 == 0
        and kb >= zs
    )


def cas_of(product, length):
    angle = (product & (length - 1)).astype(F32) * (2.0 * math.pi / length)
    return jnp.cos(angle) + jnp.sin(angle)


def spectral(density, green, groups, pencils, scale):
    n, pens = groups, pencils
    zs, xl, y = density.shape
    kb, yl, u = green.shape
    z_all, k_all = zs * n, kb * n
    half = yl // HALVES
    rows = half // n
    lanes = 512
    strip = 32

    lag = min(LAG, zs)
    others = [*range(1, pens - 1), 0] if pens > 2 else [0]

    def kernel(d_hbm, g_hbm, out, dens, stage, gsend, grecv, ysend, yrecv, psend, precv,
               brecv, xsend, ret, ready, table, wide, tall, load, gs, gr, ys, yr, ps, pr, bs, br, xs, xr,
               done):
        g = lax.axis_index("gz")
        p = lax.axis_index("pa")

        def gz_at(i):
            return lax.rem(g + 1 + i, n)

        def pa_at(i):
            return lax.rem(p + 1 + i, pens)

        def green_load(t):
            h, i = t // n, lax.rem(t, n)
            at = pl.multiple_of(h * half + gz_at(i) * rows, rows)
            return pltpu.make_async_copy(
                g_hbm.at[:, pl.ds(at, rows), :], stage.at[lax.rem(t, 2)], load.at[lax.rem(t, 2)]
            )

        def green_cast(t):
            h, i = t // n, lax.rem(t, n)
            slot = lax.rem(t, 2)
            green_load(t).wait()

            @pl.when(i < n - 1)
            def _():
                gsend[h, gz_at(i)] = stage[slot].astype(BF)

            @pl.when(i == n - 1)
            def _():
                grecv[h, g] = stage[slot].astype(BF)

            @pl.when(t < HALVES * n - 2)
            def _():
                green_load(t + 2).start()

        def settle(ref, sem):
            pltpu.make_async_copy(ref, ref, sem).wait()

        def green_copy(h, d):
            return pltpu.make_async_remote_copy(
                gsend.at[h, d], grecv.at[h, g], gs, gr.at[h],
                device_id={"gz": d}, device_id_type=MESH)

        def y_copy(z, q):
            return pltpu.make_async_remote_copy(
                ysend.at[q, z], yrecv.at[p, z], ys, yr.at[z],
                device_id={"pa": q}, device_id_type=MESH)

        def p_copy(h, d):
            return pltpu.make_async_remote_copy(
                psend.at[h, d], precv.at[h, g], ps, pr.at[h],
                device_id={"gz": d}, device_id_type=MESH)

        def b_copy(h, z, d):
            return pltpu.make_async_remote_copy(
                gsend.at[h, d, z], brecv.at[h, z, g], bs, br.at[h, z],
                device_id={"gz": d}, device_id_type=MESH)

        def x_at(h):
            return pl.ds(pl.multiple_of(p * yl + h * half, half), half)

        def x_copy(h, z, q):
            return pltpu.make_async_remote_copy(
                xsend.at[h, z, q], ret.at[z, :, x_at(h)], xs, xr.at[z],
                device_id={"pa": q}, device_id_type=MESH)

        def y_back(z):
            settle(ret.at[z, :, 0 : (pens - 1) * yl], xr.at[z])
            slot = lax.rem(z, 2)

            @pl.when(z >= 2)
            def _():
                settle(ready.at[slot], done.at[slot])

            for at in range(0, xl, xl // 2):
                part = slice(at, at + xl // 2)
                ready[slot, part] = (dot(ret[z, part], table[...]) * scale).astype(BF)
                pltpu.make_async_copy(ready.at[slot, part], out.at[z, part], done.at[slot]).start()

        fill = pltpu.make_async_copy(d_hbm, dens, load.at[2])
        green_load(0).start()
        green_load(1).start()
        fill.start()
        barrier = pltpu.get_barrier_semaphore()

        @pl.loop(0, n - 1)
        def _(i):
            pl.semaphore_signal(barrier, inc=1, device_id={"gz": gz_at(i)}, device_id_type=MESH)

        @pl.loop(0, pens - 1)
        def _(i):
            pl.semaphore_signal(barrier, inc=1, device_id={"pa": pa_at(i)}, device_id_type=MESH)

        green_cast(jnp.int32(0))
        pl.semaphore_wait(barrier, n + pens - 2)

        @pl.loop(0, HALVES * n)
        def _(t):
            h, i = t // n, lax.rem(t, n)

            @pl.when(i < n - 1)
            def _():
                green_copy(h, gz_at(i)).start()

            @pl.when(t < HALVES * n - 1)
            def _():
                green_cast(t + 1)

        @pl.loop(0, y // strip)
        def _(b):
            row = lax.broadcasted_iota(jnp.int32, (strip, y), 0) + b * strip
            col = lax.broadcasted_iota(jnp.int32, (strip, y), 1)
            table[pl.ds(pl.multiple_of(b * strip, strip), strip), :] = cas_of(row * col, y).astype(BF)

        fill.wait()

        @pl.loop(0, zs)
        def _(z):
            for q in range(pens):
                ysend[q, z] = dot_t(table[q * yl : (q + 1) * yl, :], dens[z]).astype(BF)

            @pl.loop(0, pens - 1)
            def _(i):
                y_copy(z, pa_at(i)).start()

            yrecv[p, z] = ysend[p, z]

        def widen(ref):
            shape = (strip, ref.shape[1])

            @pl.loop(0, ref.shape[0] // strip)
            def _(b):
                row = lax.broadcasted_iota(jnp.int32, shape, 0) + b * strip
                col = lax.broadcasted_iota(jnp.int32, shape, 1)
                value = cas_of((row >> 3) * (col >> 3), k_all)
                same = (row & 7) == (col & 7)
                ref[pl.ds(pl.multiple_of(b * strip, strip), strip), :] = jnp.where(same, value, 0.0).astype(BF)

        widen(wide)
        widen(tall)

        @pl.loop(0, zs)
        def _(z):
            settle(yrecv.at[0 : pens - 1, z], yr.at[z])

            total = dot(yrecv[0, z], table[0:xl, :])
            for q in range(1, pens):
                total += dot(yrecv[q, z], table[q * xl : (q + 1) * xl, :])
            total = total.astype(BF)
            for h in range(HALVES):
                for d in range(n):
                    at = h * half + d * rows
                    psend[h, d, z] = total[at : at + rows, :]

        for h in range(HALVES):
            @pl.loop(0, n - 1)
            def _(i):
                p_copy(h, gz_at(i)).start()

            precv[h, g] = psend[h, g]

        settle(gsend.at[:, 0 : n - 1], gs)
        for h in range(HALVES):
            settle(grecv.at[h, 0 : n - 1], gr.at[h])
            settle(precv.at[h, 0 : n - 1], pr.at[h])

            @pl.loop(0, u // lanes)
            def _(c):
                at = pl.ds(pl.multiple_of(c * lanes, lanes), lanes)
                for r in range(0, rows, 8):
                    part = slice(r, r + 8)
                    flat = precv[h, :, :, part, at].astype(F32).reshape(z_all * 8, lanes).astype(BF)
                    spec = dot(wide[...], flat)
                    weight = grecv[h, :, :, part, at].astype(F32).reshape(k_all * 8, lanes)
                    back = dot(tall[...], (spec * weight).astype(BF))
                    gsend[h, :, :zs, part, at] = back.reshape(n, zs, 8, lanes).astype(BF)

            @pl.loop(0, zs)
            def _(z):
                @pl.loop(0, n - 1)
                def _(i):
                    b_copy(h, z, gz_at(i)).start()

                brecv[h, z, g] = gsend[h, g, z]

        @pl.loop(0, HALVES * zs)
        def _(t):
            h, z = t // zs, lax.rem(t, zs)
            settle(brecv.at[h, z, 0 : n - 1], br.at[h, z])
            rows_in = brecv[h, z].reshape(half, u)

            def piece(q):
                at = pl.ds(pl.multiple_of(q * xl, xl), xl)
                return dot_t(table[at, :], rows_in).astype(BF)

            for at, i in enumerate(others):
                xsend[h, z, pa_at(i)] = piece(pa_at(i))
                if at:
                    x_copy(h, z, pa_at(others[at - 1])).start()
            ret[z, :, x_at(h)] = piece(p)
            x_copy(h, z, pa_at(others[-1])).start()

            @pl.when((h == HALVES - 1) & (z >= lag))
            def _():
                y_back(z - lag)

        for z in range(zs - lag, zs):
            y_back(jnp.int32(z))
        settle(ysend.at[0 : pens - 1], ys)
        settle(psend.at[:, 0 : n - 1], ps)
        settle(gsend.at[:, 0 : n - 1, 0:zs], bs)
        settle(xsend.at[:, :, 0 : pens - 1], xs)
        for z in range(max(zs - 2, 0), zs):
            settle(ready.at[z % 2], done.at[z % 2])

    sems = pltpu.SemaphoreType.DMA
    return pl.pallas_call(
        kernel,
        out_shape=jax.ShapeDtypeStruct((zs, xl, y), BF),
        in_specs=[pl.BlockSpec(memory_space=pl.ANY)] * 2,
        out_specs=pl.BlockSpec(memory_space=pl.ANY),
        scratch_shapes=[
            pltpu.VMEM((zs, xl, y), BF),
            pltpu.VMEM((2, kb, rows, u), F32),
            pltpu.VMEM((HALVES, n, kb, rows, u), BF),
            pltpu.VMEM((HALVES, n, kb, rows, u), BF),
            pltpu.VMEM((pens, zs, yl, xl), BF),
            pltpu.VMEM((pens, zs, yl, xl), BF),
            pltpu.VMEM((HALVES, n, zs, rows, u), BF),
            pltpu.VMEM((HALVES, n, zs, rows, u), BF),
            pltpu.VMEM((HALVES, zs, n, rows, u), BF),
            pltpu.VMEM((HALVES, zs, pens, xl, half), BF),
            pltpu.VMEM((zs, xl, y), BF),
            pltpu.VMEM((2, xl, y), BF),
            pltpu.VMEM((y, y), BF),
            pltpu.VMEM((k_all * 8, z_all * 8), BF),
            pltpu.VMEM((z_all * 8, k_all * 8), BF),
            sems((3,)),
            sems,
            sems((HALVES,)),
            sems,
            sems((zs,)),
            sems,
            sems((HALVES,)),
            sems,
            sems((HALVES, zs)),
            sems,
            sems((zs,)),
            sems((2,)),
        ],
        compiler_params=pltpu.CompilerParams(
            collective_id=0, has_side_effects=True, vmem_limit_bytes=67_000_000
        ),
        name="spectral",
    )(density, green)


def widen_result(narrow):
    z, x, y = narrow.shape

    def body(n_hbm, o_hbm, held, made, arrive, leave):
        def taken(i):
            return pltpu.make_async_copy(n_hbm.at[i], held.at[i], arrive.at[i])

        def given(i):
            return pltpu.make_async_copy(made.at[i], o_hbm.at[i], leave.at[i])

        for i in range(z):
            taken(i).start()
        for i in range(z):
            taken(i).wait()
            made[i] = held[i].astype(F32)
            given(i).start()
        for i in range(z):
            given(i).wait()

    sems = pltpu.SemaphoreType.DMA
    return pl.pallas_call(
        body,
        in_specs=[pl.BlockSpec(memory_space=pl.ANY)],
        out_specs=pl.BlockSpec(memory_space=pl.ANY),
        out_shape=jax.ShapeDtypeStruct((z, x, y), F32),
        scratch_shapes=[
            pltpu.VMEM((z, x, y), BF),
            pltpu.VMEM((z, x, y), F32),
            sems((z,)),
            sems((z,)),
        ],
        compiler_params=pltpu.CompilerParams(vmem_limit_bytes=67_000_000),
        cost_estimate=cost(z * x * y, narrow, narrow, narrow),
        name="widen_result",
    )(narrow)


def local(density, green):
    groups = lax.axis_size("gz")
    pencils = lax.axis_size("pa")
    if not fits(density, green, groups, pencils):
        return staged(density, green)
    scale = 1.0 / (green.shape[2] * density.shape[2] * green.shape[0] * groups)
    return widen_result(spectral(density, green, groups, pencils, scale))


def solution(mesh):
    return jax.shard_map(
        local,
        mesh=mesh,
        in_specs=(P("gz", "pa", None), P("gz", "pa", None)),
        out_specs=P("gz", "pa", None),
        check_vma=False,
    )
```
